512 devices in a mesh: seq: 64 (over z, y_hi, core), head: 8 (over y_lo, x).
Axes of the slice: x: 4, y: 8 (y_hi: 4, y_lo: 2; y = y_hi * 2 + y_lo), z: 8, core: 2. Of those that a mesh axis runs over, the one named last changes fastest.
Arguments:
- qkv: bfloat16 [3, 8192, 4096], P(None, ('seq', 'head')), may hold values from -128 to 128
- token_rate: float32 [8192, 8], P('seq', 'head'), may hold values from 0.1 to 1
- head_rate: float32 [8], P('head'), may hold values from 0.5 to 2
- fast_state: float32 [3, 8, 512, 512], P(None, 'head', 'seq'), may hold values from -0.25 to 0.25
Outputs:
- combined: bfloat16 [8192, 4096], P(('seq', 'head'))
- new_state: float32 [3, 8, 512, 512], P(None, 'head', 'seq')
The draws below stay inside these ranges and needn't reach their ends.
All inputs are finite; a program needn't handle non-finite values.
Results may differ from the reference program's by a relative error of at most 0.017.
Values may be sent and summed in bfloat16 or wider, within the bound.
No kernel may reach another device: no remote copies, remote signals or barrier semaphores. Data moves between devices by JAX's collectives and lax.ppermute only.
A program may use at most 64 MiB of HBM per device.

```python
import math
import jax
import jax.numpy as jnp
from jax import lax

HD = 512
FH = 512
HEADS = 8
TOK_DEV = 128
TOKENS = 8192
WINDOW = 1024
NS_STEPS = 2


def draw_qkv(key, part):
    feature_count = HEADS * HD
    branches = jax.random.split(key, 1)
    drawn = jnp.clip(jax.random.normal(branches[0], (3, TOKENS, feature_count), jnp.float32), -6.0, 6.0)
    drawn = drawn * jnp.array([1.0, 1.0, 2.0], jnp.float32)[:, None, None]
    return drawn.astype(jnp.bfloat16)


def steps_of(key, shape, cuts, smallest, high):
    level = 1.0
    for position, blocks in cuts:
        steps = jax.random.uniform(jax.random.fold_in(jax.random.fold_in(key, 6), position), (blocks,), jnp.float32, smallest / len(cuts), high / len(cuts))
        level = level * jnp.repeat(jnp.exp(steps), shape[position] // blocks).reshape((-1,) + (1,) * (len(shape) - 1 - position))
    return level


def bell_draw(rng, shape, width, limit, cuts=(), kind=jnp.bfloat16):
    loudness = steps_of(rng, shape, cuts, -0.22, 0.18) if cuts else 1.0
    values = jax.random.normal(rng, shape, jnp.float32) * width * loudness
    return jnp.minimum(jnp.maximum(values, -limit), limit).astype(kind)


def setup_inputs(seed: int = 0) -> dict:
    streams_of = jax.random.split(jax.random.key(seed), 5)
    qkv = draw_qkv(jax.random.fold_in(streams_of[4], 71), 0)
    token_rate = jnp.clip(jnp.exp(math.log(1.0) - 2.3025851 * jax.random.uniform(streams_of[1], (TOKENS, HEADS), jnp.float32) ** steps_of(streams_of[1], (TOKENS, HEADS), ((0, 64), (1, 8)), -0.2, 0.2)), 0.1, 1.0)
    head_rate = jnp.clip(jnp.exp(math.log(2.0) - 1.3862944 * jax.random.uniform(streams_of[2], (HEADS,), jnp.float32) ** steps_of(streams_of[2], (HEADS,), ((0, 8),), -0.2, 0.2)), 0.5, 2.0)
    fast_state = bell_draw(streams_of[3], (3, HEADS, FH, HD), HD ** -0.5, 0.25, ((1, 8), (2, 64)), jnp.float32)
    return {"qkv": qkv, "token_rate": token_rate, "head_rate": head_rate, "fast_state": fast_state}


ns_first = 3.4445
ns_second = -4.775
ns_third = 2.0315
rms_eps = 1e-06
norm_eps = 1e-07
precise = lax.Precision.HIGHEST

def rms_scaled(values):
    return values * lax.rsqrt(lax.optimization_barrier(jnp.mean(values * values, axis=-1, keepdims=True)) + rms_eps)

def contract_last(left_side, right_side):
    return lax.dot_general(left_side, right_side, (((1,), (1,)), ((), ())), preferred_element_type=jnp.float32)

def contract_first(left_side, right_side):
    return lax.dot_general(left_side, right_side, (((0,), (0,)), ((), ())), preferred_element_type=jnp.float32)

def head_gradient(key_norm, signal, weight_piece):
    gate_act = contract_last(key_norm, weight_piece[0])
    up_act = contract_last(key_norm, weight_piece[1])
    active = (jax.nn.silu(gate_act) * up_act).astype(jnp.bfloat16)
    back_grad = contract_last(signal, weight_piece[2])
    sigmoid_gate = jax.nn.sigmoid(gate_act)
    grad_gate = (back_grad * up_act * sigmoid_gate * (1.0 + gate_act * (1.0 - sigmoid_gate))).astype(jnp.bfloat16)
    grad_up = (back_grad * jax.nn.silu(gate_act)).astype(jnp.bfloat16)
    return jnp.stack([contract_first(grad_gate, key_norm), contract_first(grad_up, key_norm), contract_first(active, signal)])

def window_attention(queries, keys_head, values_head):
    pad_rows = jnp.zeros((WINDOW, HD), jnp.bfloat16)
    padded_keys = jnp.concatenate([pad_rows, keys_head], axis=0)
    padded_values = jnp.concatenate([pad_rows, values_head], axis=0)
    starts = jnp.arange(TOKENS // TOK_DEV, dtype=jnp.int32) * TOK_DEV

    def one_block(block_start):
        query_block = lax.dynamic_slice_in_dim(queries, block_start, TOK_DEV, 0)
        key_block = lax.dynamic_slice_in_dim(padded_keys, block_start, WINDOW + TOK_DEV, 0)
        value_block = lax.dynamic_slice_in_dim(padded_values, block_start, WINDOW + TOK_DEV, 0)
        scores = contract_last(query_block, key_block) * HD ** (-0.5)
        query_pos = block_start + jnp.arange(TOK_DEV, dtype=jnp.int32)[:, None]
        key_pos = block_start - WINDOW + jnp.arange(WINDOW + TOK_DEV, dtype=jnp.int32)[None, :]
        visible = (key_pos <= query_pos) & (key_pos > query_pos - WINDOW) & (key_pos >= 0)
        scores = jnp.where(visible, scores, -jnp.inf)
        row_max = lax.optimization_barrier(jnp.max(scores, axis=1, keepdims=True))
        exp_scores = jnp.exp(scores - row_max)
        weights = (exp_scores / lax.optimization_barrier(jnp.sum(exp_scores, axis=1, keepdims=True))).astype(jnp.bfloat16)
        return jnp.dot(weights, value_block, preferred_element_type=jnp.float32)
    return lax.map(one_block, starts).reshape(TOKENS, HD)

def newton_schulz(gradients):
    frob_norm = jnp.sqrt(lax.optimization_barrier(jnp.sum(gradients * gradients, axis=(1, 2), keepdims=True)))
    iterate = gradients / (frob_norm + norm_eps)
    for section_number in range(NS_STEPS):
        gram_matrix = jnp.einsum('mij,mkj->mik', iterate, iterate, precision=precise)
        poly_part = ns_second * gram_matrix + ns_third * jnp.einsum('mij,mjk->mik', gram_matrix, gram_matrix, precision=precise)
        iterate = ns_first * iterate + jnp.einsum('mij,mjk->mik', poly_part, iterate, precision=precise)
    return iterate

def one_head(packed):
    queries, keys_head, values_head, token_rates, step_size, head_state = packed
    query_norm = rms_scaled(queries.astype(jnp.float32)).astype(jnp.bfloat16)
    key_norm = rms_scaled(keys_head.astype(jnp.float32)).astype(jnp.bfloat16)
    signal = (-token_rates[:, None] * values_head.astype(jnp.float32)).astype(jnp.bfloat16)
    gradients = head_gradient(key_norm, signal, head_state.astype(jnp.bfloat16))
    updated = head_state - step_size * newton_schulz(gradients)
    new_low = updated.astype(jnp.bfloat16)
    gate_act = contract_last(query_norm, new_low[0])
    up_act = contract_last(query_norm, new_low[1])
    active = (jax.nn.silu(gate_act) * up_act).astype(jnp.bfloat16)
    fast_out = jnp.dot(active, new_low[2], preferred_element_type=jnp.float32)
    attention = window_attention(queries, keys_head, values_head)
    return ((attention + fast_out).astype(jnp.bfloat16), updated)

def reference(qkv, token_rate, head_rate, fast_state):
    split_heads = qkv.reshape(3, TOKENS, HEADS, HD).transpose(0, 2, 1, 3)
    outputs, states = lax.map(one_head, (split_heads[0], split_heads[1], split_heads[2], token_rate.T, head_rate, fast_state.transpose(1, 0, 2, 3)))
    combined = outputs.transpose(1, 0, 2).reshape(TOKENS, HEADS * HD)
    return (combined, states.transpose(1, 0, 2, 3))
```

```python
import jax
import jax.numpy as jnp
from jax import lax
from jax.experimental import pallas as pl
from jax.experimental.pallas import tpu as pltpu
from jax.sharding import Mesh
from jax.sharding import PartitionSpec as P

WINDOW = 1024
NS_STEPS = 2
NS_1, NS_2, NS_3 = 3.4445, -4.775, 2.0315
RMS_EPS = 1e-06
NORM_EPS = 1e-07

SEQ = ("z", "y", "core")
SEQ_HEAD = ("z", "y", "core", "head")
CHIPS = ("z", "y")
F32, BF16 = jnp.float32, jnp.bfloat16


def dot_nt(a, b):
    return lax.dot_general(a, b, (((1,), (1,)), ((), ())), preferred_element_type=F32)


def dot_nn(a, b):
    return lax.dot_general(a, b, (((1,), (0,)), ((), ())), preferred_element_type=F32)


def local_call(body, outs, args, smem=(), scratch=()):
    specs = [
        pl.BlockSpec(memory_space=pltpu.SMEM if i in smem else pltpu.VMEM) for i in range(len(args))
    ]
    single = not isinstance(outs, (list, tuple))
    out_list = [outs] if single else list(outs)
    out_specs = [pl.BlockSpec(memory_space=pltpu.VMEM) for _ in out_list]
    return pl.pallas_call(
        body,
        in_specs=specs,
        out_specs=out_specs[0] if single else out_specs,
        out_shape=outs if single else out_list,
        scratch_shapes=list(scratch),
        name=body.__name__,
    )(*args)


def split_heads(qkv_ref, out_ref):
    for h in range(out_ref.shape[0]):
        hd = out_ref.shape[3]
        for j in range(3):
            out_ref[h, j] = qkv_ref[j, :, h * hd : (h + 1) * hd]


def rms_scaled(x):
    return x * lax.rsqrt(jnp.mean(x * x, axis=-1, keepdims=True) + RMS_EPS)


def prepare(arr_ref, rate_ref, q_ref, kv_ref, qn_ref, ks_ref):
    n, _, t, _ = arr_ref.shape
    for j in range(n):
        rows = slice(j * t, (j + 1) * t)
        q, k, v = arr_ref[j, 0], arr_ref[j, 1], arr_ref[j, 2]
        q_ref[rows] = q
        kv_ref[0, rows] = k
        kv_ref[1, rows] = v
        qn_ref[rows] = rms_scaled(q.astype(F32)).astype(BF16)
        ks_ref[0, rows] = rms_scaled(k.astype(F32)).astype(BF16)
        ks_ref[1, rows] = (-rate_ref[rows] * v.astype(F32)).astype(BF16)


def copies_of(rows_ref, out_ref):
    rows = rows_ref[...].astype(BF16)
    for d in range(out_ref.shape[0]):
        out_ref[d] = rows


def merged_rows(ref, m):
    n, _, r, w = ref.shape
    return ref[:, m].astype(F32).reshape(n * r, w)


def gradient(own_ref, other_ref, w_ref, out_ref):
    n, _, r, w = w_ref.shape
    key_norm = jnp.concatenate([own_ref[0], other_ref[0]], axis=0)
    signal = jnp.concatenate([own_ref[1], other_ref[1]], axis=0)
    gate = dot_nt(merged_rows(w_ref, 0).astype(BF16), key_norm)
    up = dot_nt(merged_rows(w_ref, 1).astype(BF16), key_norm)
    back = dot_nt(merged_rows(w_ref, 2).astype(BF16), signal)
    s = jax.nn.sigmoid(gate)
    silu = gate * s
    grads = (
        ((back * up * s * (1.0 + gate * (1.0 - s))).astype(BF16), key_norm),
        ((back * silu).astype(BF16), key_norm),
        ((silu * up).astype(BF16), signal),
    )
    for m, (left, right) in enumerate(grads):
        out_ref[:, m] = dot_nn(left, right).reshape(n, r, w).astype(BF16)


def sum_and_copy(arr_ref, out_ref):
    total = arr_ref[0].astype(F32)
    for d in range(1, arr_ref.shape[0]):
        total = total + arr_ref[d].astype(F32)
    total = total.astype(BF16)
    for d in range(out_ref.shape[0]):
        out_ref[d] = total


def attend(where_ref, q_ref, own_ref, other_ref, out_ref):
    blocks, _, t, w = own_ref.shape
    chip, core = where_ref[0], where_ref[1]
    q = q_ref[...]
    q_pos = (2 * chip + core) * t + lax.broadcasted_iota(jnp.int32, (t, t), 0)
    lane = lax.broadcasted_iota(jnp.int32, (t, t), 1)
    parts = []
    for b in range(blocks):
        for ref, c in ((own_ref, core), (other_ref, 1 - core)):
            k_pos = (2 * (chip - b) + c) * t + lane
            seen = (k_pos <= q_pos) & (k_pos > q_pos - WINDOW) & (k_pos >= 0)
            scores = dot_nt(q, ref[b, 0]) * (w ** (-0.5))
            parts.append(jnp.where(seen, scores, -jnp.inf))
    top = parts[0]
    for p in parts[1:]:
        top = jnp.maximum(top, p)
    top = jnp.max(top, axis=1, keepdims=True)
    parts = [jnp.exp(p - top) for p in parts]
    total = parts[0]
    for p in parts[1:]:
        total = total + p
    inverse = 1.0 / jnp.sum(total, axis=1, keepdims=True)
    out = jnp.zeros((t, w), F32)
    for b in range(blocks):
        for i, ref in enumerate((own_ref, other_ref)):
            out = out + dot_nn((parts[2 * b + i] * inverse).astype(BF16), ref[b, 1])
    out_ref[...] = out


def finish(
    where_ref, rate_ref, g_own, g_other, old_own, old_other, state_ref, qn_ref, att_ref,
    rows_ref, out_ref, x_ref, fresh_ref,
):
    n, _, r, _ = g_own.shape
    half = n * r
    rate = rate_ref[0]
    chip = where_ref[0]

    def one_matrix(m, carry):
        g = jnp.concatenate([merged_rows(g_own, m), merged_rows(g_other, m)], axis=0)
        norm = jnp.sqrt(jnp.sum(g * g, keepdims=True))
        x = g / (norm + NORM_EPS)
        for _ in range(NS_STEPS):
            low = x.astype(BF16)
            gram = dot_nt(low, low)
            gram_low = gram.astype(BF16)
            poly = NS_2 * gram + NS_3 * dot_nn(gram_low, gram_low)
            x = NS_1 * x + dot_nn(poly.astype(BF16), low)
        x_ref[...] = x
        fresh_ref[m, :half] = (merged_rows(old_own, m) - rate * x[:half]).astype(BF16)
        fresh_ref[m, half:] = (merged_rows(old_other, m) - rate * x[half:]).astype(BF16)
        rows_ref[m] = state_ref[m] - rate * x_ref[pl.ds(pl.multiple_of(chip * r, r), r)]
        return carry

    lax.fori_loop(0, 3, one_matrix, 0)
    gate = dot_nt(qn_ref[...], fresh_ref[0])
    up = dot_nt(qn_ref[...], fresh_ref[1])
    active = (jax.nn.silu(gate) * up).astype(BF16)
    out_ref[...] = (att_ref[...] + dot_nn(active, fresh_ref[2])).astype(BF16)


def join_heads(arr_ref, out_ref):
    for h in range(arr_ref.shape[0]):
        hd = arr_ref.shape[2]
        out_ref[:, h * hd : (h + 1) * hd] = arr_ref[h]


def shards(qkv, token_rate, head_rate, fast_state):
    heads = lax.axis_size("head")
    chips = lax.axis_size("z") * lax.axis_size("y")
    _, tok_part, width = qkv.shape
    hd = width // heads
    tok = tok_part * heads
    rows = fast_state.shape[2]
    chip = lax.axis_index(CHIPS)
    core = lax.axis_index("core")
    where = jnp.stack([chip, core]).astype(jnp.int32)
    state = fast_state[:, 0]
    swap = [(0, 1), (1, 0)]

    def shape(dims, dtype=BF16):
        return jax.ShapeDtypeStruct(dims, dtype)

    def exchanged(pieces, axis):
        return lax.all_to_all(pieces, axis, 0, 0, tiled=True)

    old_copies = local_call(copies_of, shape((chips, 3, rows, hd)), (state,))
    split = local_call(split_heads, shape((heads, 3, tok_part, hd)), (qkv,))
    arrived = exchanged(split, "head")
    old_own = exchanged(old_copies, CHIPS)
    q, kv, q_norm, ks = local_call(
        prepare,
        [shape((tok, hd)), shape((2, tok, hd)), shape((tok, hd)), shape((2, tok, hd))],
        (arrived, token_rate),
    )
    ks_other = lax.ppermute(ks, "core", swap)
    before = WINDOW // (2 * tok)
    own_blocks = [kv] + [
        lax.ppermute(kv, CHIPS, [(i - d, i) for i in range(d, chips)]) for d in range(1, before + 1)
    ]
    own_kv = jnp.stack(own_blocks)
    partial = local_call(gradient, shape((chips, 3, rows, hd)), (ks, ks_other, old_own))
    parts = exchanged(partial, CHIPS)
    g_copies = local_call(sum_and_copy, shape((chips, 3, rows, hd)), (parts,))
    g_own = exchanged(g_copies, CHIPS)
    other_kv = lax.ppermute(own_kv, "core", swap)
    attention = local_call(attend, shape((tok, hd), F32), (where, q, own_kv, other_kv), smem=(0,))
    old_other = lax.ppermute(old_own, "core", swap)
    g_other = lax.ppermute(g_own, "core", swap)
    new_rows, combined = local_call(
        finish,
        [shape((3, rows, hd), F32), shape((tok, hd))],
        (where, head_rate, g_own, g_other, old_own, old_other, state, q_norm, attention),
        smem=(0, 1),
        scratch=[
            pltpu.VMEM((2 * chips * rows, hd), F32),
            pltpu.VMEM((3, 2 * chips * rows, hd), BF16),
        ],
    )
    back = exchanged(combined.reshape(heads, tok_part, hd), "head")
    return (
        local_call(join_heads, shape((tok_part, width)), (back,)),
        new_rows[:, None],
    )


def solution(mesh):
    finer = Mesh(mesh.devices.reshape(8, 4, 2, mesh.shape["head"]), SEQ_HEAD)
    return jax.shard_map(
        shards,
        mesh=finer,
        in_specs=(P(None, SEQ_HEAD, None), P(SEQ, "head"), P("head"), P(None, "head", SEQ, None)),
        out_specs=(P(SEQ_HEAD, None), P(None, "head", SEQ, None)),
        check_vma=False,
    )
```

```python
import jax
import jax.numpy as jnp
from jax import lax
from jax.experimental import pallas as pl
from jax.experimental.pallas import tpu as pltpu
from jax.sharding import Mesh
from jax.sharding import PartitionSpec as P

WINDOW = 1024
NS_STEPS = 2
NS_1, NS_2, NS_3 = 3.4445, -4.775, 2.0315
RMS_EPS = 1e-06
NORM_EPS = 1e-07

SEQ = ("z", "y", "core")
SEQ_HEAD = ("z", "y", "core", "head")
CHIPS = ("z", "y")
F32, BF16 = jnp.float32, jnp.bfloat16
KERNEL_VMEM = 20 * 1024 * 1024


def dot_nt(a, b):
    return lax.dot_general(a, b, (((1,), (1,)), ((), ())), preferred_element_type=F32)


def dot_nn(a, b):
    return lax.dot_general(a, b, (((1,), (0,)), ((), ())), preferred_element_type=F32)


def local_call(body, outs, args, smem=(), scratch=(), hbm_in=(), hbm_out=()):
    specs = [
        pl.BlockSpec(memory_space=pltpu.SMEM if i in smem else pltpu.VMEM) for i in range(len(args))
    ]
    single = not isinstance(outs, (list, tuple))
    out_list = [outs] if single else list(outs)
    out_list = [
        o if i in hbm_out else pltpu.VMEM(o.shape, o.dtype) for i, o in enumerate(out_list)
    ]
    args = [
        a if i in smem or i in hbm_in else pltpu.with_memory_space_constraint(a, pltpu.VMEM)
        for i, a in enumerate(args)
    ]
    out_specs = [pl.BlockSpec(memory_space=pltpu.VMEM) for _ in out_list]
    return pl.pallas_call(
        body,
        in_specs=specs,
        out_specs=out_specs[0] if single else out_specs,
        out_shape=out_list[0] if single else out_list,
        scratch_shapes=list(scratch),
        compiler_params=pltpu.CompilerParams(vmem_limit_bytes=KERNEL_VMEM),
    )(*args)


def split_heads(where_ref, qkv_ref, *out_refs):
    hd = out_refs[0].shape[2]
    for d, out_ref in enumerate(out_refs):
        start = pl.multiple_of((where_ref[2] ^ d) * hd, hd)
        for j in range(3):
            out_ref[j] = qkv_ref[j, :, pl.ds(start, hd)]


def rms_scaled(x):
    return x * lax.rsqrt(jnp.mean(x * x, axis=-1, keepdims=True) + RMS_EPS)


def prepare(where_ref, rate_ref, *refs):
    pieces, (q_ref, kv_ref, qn_ref, ks_ref) = refs[:-4], refs[-4:]
    t = pieces[0].shape[1]
    for d, piece in enumerate(pieces):
        rows = pl.ds(pl.multiple_of((where_ref[2] ^ d) * t, t), t)
        q, k, v = piece[0], piece[1], piece[2]
        q_ref[rows] = q
        kv_ref[0, rows] = k
        kv_ref[1, rows] = v
        qn_ref[rows] = rms_scaled(q.astype(F32)).astype(BF16)
        ks_ref[0, rows] = rms_scaled(k.astype(F32)).astype(BF16)
        ks_ref[1, rows] = (-rate_ref[rows] * v.astype(F32)).astype(BF16)


def copies_of(rows_ref, out_ref):
    rows = rows_ref[...].astype(BF16)
    for d in range(out_ref.shape[0]):
        out_ref[d] = rows


def merged_rows(ref, m):
    n, _, r, w = ref.shape
    return ref[:, m].astype(F32).reshape(n * r, w)


def gradient(own_ref, other_ref, w_ref, out_ref):
    n, _, r, w = w_ref.shape
    key_norm = jnp.concatenate([own_ref[0], other_ref[0]], axis=0)
    signal = jnp.concatenate([own_ref[1], other_ref[1]], axis=0)
    gate = dot_nt(merged_rows(w_ref, 0).astype(BF16), key_norm)
    up = dot_nt(merged_rows(w_ref, 1).astype(BF16), key_norm)
    back = dot_nt(merged_rows(w_ref, 2).astype(BF16), signal)
    s = jax.nn.sigmoid(gate)
    silu = gate * s
    grads = (
        ((back * up * s * (1.0 + gate * (1.0 - s))).astype(BF16), key_norm),
        ((back * silu).astype(BF16), key_norm),
        ((silu * up).astype(BF16), signal),
    )
    for m, (left, right) in enumerate(grads):
        out_ref[:, m] = dot_nn(left, right).reshape(n, r, w).astype(BF16)


def sum_and_copy(arr_ref, out_ref):
    total = arr_ref[0].astype(F32)
    for d in range(1, arr_ref.shape[0]):
        total = total + arr_ref[d].astype(F32)
    total = total.astype(BF16)
    for d in range(out_ref.shape[0]):
        out_ref[d] = total


def attend(where_ref, q_ref, own_ref, other_ref, out_ref):
    blocks, _, t, w = own_ref.shape
    chip, core = where_ref[0], where_ref[1]
    q = q_ref[...]
    q_pos = (2 * chip + core) * t + lax.broadcasted_iota(jnp.int32, (t, t), 0)
    lane = lax.broadcasted_iota(jnp.int32, (t, t), 1)
    parts = []
    for b in range(blocks):
        for ref, c in ((own_ref, core), (other_ref, 1 - core)):
            k_pos = (2 * (chip - b) + c) * t + lane
            seen = (k_pos <= q_pos) & (k_pos > q_pos - WINDOW) & (k_pos >= 0)
            scores = dot_nt(q, ref[b, 0]) * (w ** (-0.5))
            parts.append(jnp.where(seen, scores, -jnp.inf))
    top = parts[0]
    for p in parts[1:]:
        top = jnp.maximum(top, p)
    top = jnp.max(top, axis=1, keepdims=True)
    parts = [jnp.exp(p - top) for p in parts]
    total = parts[0]
    for p in parts[1:]:
        total = total + p
    inverse = 1.0 / jnp.sum(total, axis=1, keepdims=True)
    out = jnp.zeros((t, w), F32)
    for b in range(blocks):
        for i, ref in enumerate((own_ref, other_ref)):
            out = out + dot_nn((parts[2 * b + i] * inverse).astype(BF16), ref[b, 1])
    out_ref[...] = out


def finish(
    where_ref, rate_ref, g_own, g_other, old_own, old_other, state_ref, qn_ref, att_ref,
    rows_ref, out_ref, x_ref, fresh_ref,
):
    n, _, r, _ = g_own.shape
    half = n * r
    rate = rate_ref[0]
    chip = where_ref[0]

    xs = []
    for m in range(3):
        g = jnp.concatenate([merged_rows(g_own, m), merged_rows(g_other, m)], axis=0)
        xs.append(g / (jnp.sqrt(jnp.sum(g * g, keepdims=True)) + NORM_EPS))
    for _ in range(NS_STEPS):
        lows = [x.astype(BF16) for x in xs]
        grams = [dot_nt(low, low) for low in lows]
        gram_lows = [gram.astype(BF16) for gram in grams]
        squares = [dot_nn(gram, gram) for gram in gram_lows]
        polys = [(NS_2 * gram + NS_3 * sq).astype(BF16) for gram, sq in zip(grams, squares)]
        moved = [dot_nn(poly, low) for poly, low in zip(polys, lows)]
        xs = [NS_1 * x + move for x, move in zip(xs, moved)]
    for m, x in enumerate(xs):
        fresh_ref[m, :half] = (merged_rows(old_own, m) - rate * x[:half]).astype(BF16)
        fresh_ref[m, half:] = (merged_rows(old_other, m) - rate * x[half:]).astype(BF16)
        x_ref[m] = x[:half]
        rows_ref[m] = state_ref[m] - rate * x_ref[m, pl.ds(pl.multiple_of(chip * r, r), r)]
    gate = dot_nt(qn_ref[...], fresh_ref[0])
    up = dot_nt(qn_ref[...], fresh_ref[1])
    active = (jax.nn.silu(gate) * up).astype(BF16)
    out_ref[...] = (att_ref[...] + dot_nn(active, fresh_ref[2])).astype(BF16)


def join_heads(arr_ref, out_ref):
    for h in range(arr_ref.shape[0]):
        hd = arr_ref.shape[2]
        out_ref[:, h * hd : (h + 1) * hd] = arr_ref[h]


def shards(qkv, token_rate, head_rate, fast_state):
    heads = lax.axis_size("head")
    chips = lax.axis_size("z") * lax.axis_size("y")
    _, tok_part, width = qkv.shape
    hd = width // heads
    tok = tok_part * heads
    rows = fast_state.shape[2]
    chip = lax.axis_index(CHIPS)
    core = lax.axis_index("core")
    where = jnp.stack([chip, core, lax.axis_index("head")]).astype(jnp.int32)
    state = fast_state[:, 0]
    swap = [(0, 1), (1, 0)]

    def shape(dims, dtype=BF16):
        return jax.ShapeDtypeStruct(dims, dtype)

    def exchanged(pieces, axis):
        return lax.all_to_all(pieces, axis, 0, 0, tiled=True)

    def behind(distance):
        return [(i, (i + distance) % chips) for i in range(chips)]

    old_copies = local_call(copies_of, shape((chips, 3, rows, hd)), (state,), hbm_out=(0,))
    split = local_call(
        split_heads, [shape((3, tok_part, hd))] * heads, (where, qkv), smem=(0,), hbm_in=(1,)
    )
    old_own = exchanged(old_copies, CHIPS)
    pieces = [split[0]] + [
        lax.ppermute(split[d], "head", [(i, i ^ d) for i in range(heads)])
        for d in range(1, heads)
    ]
    q, kv, q_norm, ks = local_call(
        prepare,
        [shape((tok, hd)), shape((2, tok, hd)), shape((tok, hd)), shape((2, tok, hd))],
        (where, token_rate, *pieces),
        smem=(0,),
    )
    ks_other = lax.ppermute(ks, "core", swap)
    one = lax.ppermute(kv, CHIPS, behind(1))
    three = lax.ppermute(kv, CHIPS, behind(3))
    four = lax.ppermute(kv, CHIPS, behind(4))
    two = lax.ppermute(one, CHIPS, behind(1))
    own_kv = jnp.stack([kv, one, two, three, four])
    partial = local_call(gradient, shape((chips, 3, rows, hd)), (ks, ks_other, old_own), hbm_out=(0,))
    parts = exchanged(partial, CHIPS)
    g_copies = local_call(sum_and_copy, shape((chips, 3, rows, hd)), (parts,), hbm_out=(0,))
    g_own = exchanged(g_copies, CHIPS)
    other_kv = lax.ppermute(own_kv, "core", swap)
    attention = local_call(attend, shape((tok, hd), F32), (where, q, own_kv, other_kv), smem=(0,))
    old_other = lax.ppermute(old_own, "core", swap)
    g_other = lax.ppermute(g_own, "core", swap)
    new_rows, combined = local_call(
        finish,
        [shape((3, rows, hd), F32), shape((tok, hd))],
        (where, head_rate, g_own, g_other, old_own, old_other, state, q_norm, attention),
        smem=(0, 1),
        hbm_out=(0, 1),
        scratch=[
            pltpu.VMEM((3, chips * rows, hd), F32),
            pltpu.VMEM((3, 2 * chips * rows, hd), BF16),
        ],
    )
    back = exchanged(combined.reshape(heads, tok_part, hd), "head")
    return (
        local_call(join_heads, shape((tok_part, width)), (back,), hbm_out=(0,)),
        new_rows[:, None],
    )


def solution(mesh):
    finer = Mesh(mesh.devices.reshape(8, 4, 2, mesh.shape["head"]), SEQ_HEAD)
    return jax.shard_map(
        shards,
        mesh=finer,
        in_specs=(P(None, SEQ_HEAD, None), P(SEQ, "head"), P("head"), P(None, "head", SEQ, None)),
        out_specs=(P(SEQ_HEAD, None), P(None, "head", SEQ, None)),
        check_vma=False,
    )
```

```python
import jax
import jax.numpy as jnp
from jax import lax
from jax.experimental import pallas as pl
from jax.experimental.pallas import tpu as pltpu
from jax.sharding import Mesh
from jax.sharding import PartitionSpec as P

WINDOW = 1024
NS_STEPS = 2
NS_1, NS_2, NS_3 = 3.4445, -4.775, 2.0315
RMS_EPS = 1e-06
NORM_EPS = 1e-07

SEQ = ("z", "y", "core")
SEQ_HEAD = ("z", "y", "core", "head")
CHIPS = ("z", "y")
F32, BF16 = jnp.float32, jnp.bfloat16
KERNEL_VMEM = 20 * 1024 * 1024


def dot_nt(a, b):
    return lax.dot_general(a, b, (((1,), (1,)), ((), ())), preferred_element_type=F32)


def dot_nn(a, b):
    return lax.dot_general(a, b, (((1,), (0,)), ((), ())), preferred_element_type=F32)


def local_call(body, outs, args, smem=(), scratch=(), hbm_in=(), hbm_out=()):
    specs = [
        pl.BlockSpec(memory_space=pltpu.SMEM if i in smem else pltpu.VMEM) for i in range(len(args))
    ]
    single = not isinstance(outs, (list, tuple))
    out_list = [outs] if single else list(outs)
    out_list = [
        o if i in hbm_out else pltpu.VMEM(o.shape, o.dtype) for i, o in enumerate(out_list)
    ]
    args = [
        a if i in smem or i in hbm_in else pltpu.with_memory_space_constraint(a, pltpu.VMEM)
        for i, a in enumerate(args)
    ]
    out_specs = [pl.BlockSpec(memory_space=pltpu.VMEM) for _ in out_list]
    return pl.pallas_call(
        body,
        in_specs=specs,
        out_specs=out_specs[0] if single else out_specs,
        out_shape=out_list[0] if single else out_list,
        scratch_shapes=list(scratch),
        compiler_params=pltpu.CompilerParams(vmem_limit_bytes=KERNEL_VMEM),
    )(*args)


def split_heads(qkv_ref, out_ref):
    for h in range(out_ref.shape[0]):
        hd = out_ref.shape[3]
        for j in range(3):
            out_ref[h, j] = qkv_ref[j, :, h * hd : (h + 1) * hd]


def rms_scaled(x):
    return x * lax.rsqrt(jnp.mean(x * x, axis=-1, keepdims=True) + RMS_EPS)


def prepare(arr_ref, rate_ref, q_ref, kv_ref, qn_ref, ks_ref):
    n, _, t, _ = arr_ref.shape
    for j in range(n):
        rows = slice(j * t, (j + 1) * t)
        q, k, v = arr_ref[j, 0], arr_ref[j, 1], arr_ref[j, 2]
        q_ref[rows] = q
        kv_ref[0, rows] = k
        kv_ref[1, rows] = v
        qn_ref[rows] = rms_scaled(q.astype(F32)).astype(BF16)
        ks_ref[0, rows] = rms_scaled(k.astype(F32)).astype(BF16)
        ks_ref[1, rows] = (-rate_ref[rows] * v.astype(F32)).astype(BF16)


def copies_of(rows_ref, out_ref):
    rows = rows_ref[...].astype(BF16)
    for d in range(out_ref.shape[0]):
        out_ref[d] = rows


def merged_rows(ref, m):
    n, _, r, w = ref.shape
    return ref[:, m].astype(F32).reshape(n * r, w)


def gradient(own_ref, other_ref, w_ref, out_ref):
    n, _, r, w = w_ref.shape
    key_norm = jnp.concatenate([own_ref[0], other_ref[0]], axis=0)
    signal = jnp.concatenate([own_ref[1], other_ref[1]], axis=0)
    gate = dot_nt(merged_rows(w_ref, 0).astype(BF16), key_norm)
    up = dot_nt(merged_rows(w_ref, 1).astype(BF16), key_norm)
    back = dot_nt(merged_rows(w_ref, 2).astype(BF16), signal)
    s = jax.nn.sigmoid(gate)
    silu = gate * s
    grads = (
        ((back * up * s * (1.0 + gate * (1.0 - s))).astype(BF16), key_norm),
        ((back * silu).astype(BF16), key_norm),
        ((silu * up).astype(BF16), signal),
    )
    for m, (left, right) in enumerate(grads):
        out_ref[:, m] = dot_nn(left, right).reshape(n, r, w).astype(BF16)


def sum_and_copy(arr_ref, out_ref):
    total = arr_ref[0].astype(F32)
    for d in range(1, arr_ref.shape[0]):
        total = total + arr_ref[d].astype(F32)
    total = total.astype(BF16)
    for d in range(out_ref.shape[0]):
        out_ref[d] = total


def attend(where_ref, q_ref, own_ref, other_ref, out_ref):
    blocks, _, t, w = own_ref.shape
    chip, core = where_ref[0], where_ref[1]
    q = q_ref[...]
    q_pos = (2 * chip + core) * t + lax.broadcasted_iota(jnp.int32, (t, t), 0)
    lane = lax.broadcasted_iota(jnp.int32, (t, t), 1)
    parts = []
    for b in range(blocks):
        for ref, c in ((own_ref, core), (other_ref, 1 - core)):
            k_pos = (2 * (chip - b) + c) * t + lane
            seen = (k_pos <= q_pos) & (k_pos > q_pos - WINDOW) & (k_pos >= 0)
            scores = dot_nt(q, ref[b, 0]) * (w ** (-0.5))
            parts.append(jnp.where(seen, scores, -jnp.inf))
    top = parts[0]
    for p in parts[1:]:
        top = jnp.maximum(top, p)
    top = jnp.max(top, axis=1, keepdims=True)
    parts = [jnp.exp(p - top) for p in parts]
    total = parts[0]
    for p in parts[1:]:
        total = total + p
    inverse = 1.0 / jnp.sum(total, axis=1, keepdims=True)
    out = jnp.zeros((t, w), F32)
    for b in range(blocks):
        for i, ref in enumerate((own_ref, other_ref)):
            out = out + dot_nn((parts[2 * b + i] * inverse).astype(BF16), ref[b, 1])
    out_ref[...] = out


def finish(
    where_ref, rate_ref, g_own, g_other, old_own, old_other, state_ref, qn_ref, att_ref,
    rows_ref, out_ref, x_ref, fresh_ref,
):
    n, _, r, _ = g_own.shape
    half = n * r
    rate = rate_ref[0]
    chip = where_ref[0]

    xs = []
    for m in range(3):
        g = jnp.concatenate([merged_rows(g_own, m), merged_rows(g_other, m)], axis=0)
        xs.append(g / (jnp.sqrt(jnp.sum(g * g, keepdims=True)) + NORM_EPS))
    for _ in range(NS_STEPS):
        lows = [x.astype(BF16) for x in xs]
        grams = [dot_nt(low, low) for low in lows]
        gram_lows = [gram.astype(BF16) for gram in grams]
        squares = [dot_nn(gram, gram) for gram in gram_lows]
        polys = [(NS_2 * gram + NS_3 * sq).astype(BF16) for gram, sq in zip(grams, squares)]
        moved = [dot_nn(poly, low) for poly, low in zip(polys, lows)]
        xs = [NS_1 * x + move for x, move in zip(xs, moved)]
    for m, x in enumerate(xs):
        fresh_ref[m, :half] = (merged_rows(old_own, m) - rate * x[:half]).astype(BF16)
        fresh_ref[m, half:] = (merged_rows(old_other, m) - rate * x[half:]).astype(BF16)
        x_ref[m] = x[:half]
        rows_ref[m] = state_ref[m] - rate * x_ref[m, pl.ds(pl.multiple_of(chip * r, r), r)]
    gate = dot_nt(qn_ref[...], fresh_ref[0])
    up = dot_nt(qn_ref[...], fresh_ref[1])
    active = (jax.nn.silu(gate) * up).astype(BF16)
    out_ref[...] = (att_ref[...] + dot_nn(active, fresh_ref[2])).astype(BF16)


def join_heads(arr_ref, out_ref):
    for h in range(arr_ref.shape[0]):
        hd = arr_ref.shape[2]
        out_ref[:, h * hd : (h + 1) * hd] = arr_ref[h]


def shards(qkv, token_rate, head_rate, fast_state):
    heads = lax.axis_size("head")
    chips = lax.axis_size("z") * lax.axis_size("y")
    _, tok_part, width = qkv.shape
    hd = width // heads
    tok = tok_part * heads
    rows = fast_state.shape[2]
    chip = lax.axis_index(CHIPS)
    core = lax.axis_index("core")
    where = jnp.stack([chip, core]).astype(jnp.int32)
    state = fast_state[:, 0]
    swap = [(0, 1), (1, 0)]

    def shape(dims, dtype=BF16):
        return jax.ShapeDtypeStruct(dims, dtype)

    def exchanged(pieces, axis):
        return lax.all_to_all(pieces, axis, 0, 0, tiled=True)

    def behind(distance):
        return [(i, (i + distance) % chips) for i in range(chips)]

    old_copies = local_call(copies_of, shape((chips, 3, rows, hd)), (state,), hbm_out=(0,))
    split = local_call(
        split_heads, shape((heads, 3, tok_part, hd)), (qkv,), hbm_in=(0,), hbm_out=(0,)
    )
    old_own = exchanged(old_copies, CHIPS)
    arrived = exchanged(split, "head")
    q, kv, q_norm, ks = local_call(
        prepare,
        [shape((tok, hd)), shape((2, tok, hd)), shape((tok, hd)), shape((2, tok, hd))],
        (arrived, token_rate),
    )
    ks_other = lax.ppermute(ks, "core", swap)
    one = lax.ppermute(kv, CHIPS, behind(1))
    three = lax.ppermute(kv, CHIPS, behind(3))
    four = lax.ppermute(kv, CHIPS, behind(4))
    relay = [(2 * i, 2 * j) for i, j in behind(1)] + [(2 * j + 1, 2 * i + 1) for i, j in behind(1)]
    two = lax.ppermute(jnp.where(core == 0, one, three), SEQ, relay)
    own_kv = jnp.stack([kv, one, two, three, four])
    partial = local_call(gradient, shape((chips, 3, rows, hd)), (ks, ks_other, old_own), hbm_out=(0,))
    parts = exchanged(partial, CHIPS)
    g_copies = local_call(sum_and_copy, shape((chips, 3, rows, hd)), (parts,), hbm_out=(0,))
    g_own = exchanged(g_copies, CHIPS)
    other_kv = lax.ppermute(own_kv, "core", swap)
    attention = local_call(attend, shape((tok, hd), F32), (where, q, own_kv, other_kv), smem=(0,))
    old_other = lax.ppermute(old_own, "core", swap)
    g_other = lax.ppermute(g_own, "core", swap)
    new_rows, combined = local_call(
        finish,
        [shape((3, rows, hd), F32), shape((tok, hd))],
        (where, head_rate, g_own, g_other, old_own, old_other, state, q_norm, attention),
        smem=(0, 1),
        hbm_out=(0, 1),
        scratch=[
            pltpu.VMEM((3, chips * rows, hd), F32),
            pltpu.VMEM((3, 2 * chips * rows, hd), BF16),
        ],
    )
    back = exchanged(combined.reshape(heads, tok_part, hd), "head")
    return (
        local_call(join_heads, shape((tok_part, width)), (back,), hbm_out=(0,)),
        new_rows[:, None],
    )


def solution(mesh):
    finer = Mesh(mesh.devices.reshape(8, 4, 2, mesh.shape["head"]), SEQ_HEAD)
    return jax.shard_map(
        shards,
        mesh=finer,
        in_specs=(P(None, SEQ_HEAD, None), P(SEQ, "head"), P("head"), P(None, "head", SEQ, None)),
        out_specs=(P(SEQ_HEAD, None), P(None, "head", SEQ, None)),
        check_vma=False,
    )
```

```python
import jax
import jax.numpy as jnp
from jax import lax
from jax.experimental import pallas as pl
from jax.experimental.pallas import tpu as pltpu
from jax.sharding import Mesh
from jax.sharding import PartitionSpec as P

WINDOW = 1024
NS_STEPS = 2
NS_1, NS_2, NS_3 = 3.4445, -4.775, 2.0315
RMS_EPS = 1e-06
NORM_EPS = 1e-07

SEQ = ("z", "y", "core")
SEQ_HEAD = ("z", "y", "core", "head")
CHIPS = ("z", "y")
F32, BF16 = jnp.float32, jnp.bfloat16
CHIPS_Z, CHIPS_Y = 8, 4
RATE_ROWS = 8
KERNEL_VMEM = 20 * 1024 * 1024


def dot_nt(a, b):
    return lax.dot_general(a, b, (((1,), (1,)), ((), ())), preferred_element_type=F32)


def dot_nn(a, b):
    return lax.dot_general(a, b, (((1,), (0,)), ((), ())), preferred_element_type=F32)


def local_call(body, outs, args, smem=(), scratch=(), hbm_in=(), hbm_out=()):
    specs = [
        pl.BlockSpec(memory_space=pltpu.SMEM if i in smem else pltpu.VMEM) for i in range(len(args))
    ]
    single = not isinstance(outs, (list, tuple))
    out_list = [outs] if single else list(outs)
    out_list = [
        o if i in hbm_out else pltpu.VMEM(o.shape, o.dtype) for i, o in enumerate(out_list)
    ]
    args = [
        a if i in smem or i in hbm_in else pltpu.with_memory_space_constraint(a, pltpu.VMEM)
        for i, a in enumerate(args)
    ]
    out_specs = [pl.BlockSpec(memory_space=pltpu.VMEM) for _ in out_list]
    return pl.pallas_call(
        body,
        in_specs=specs,
        out_specs=out_specs[0] if single else out_specs,
        out_shape=out_list[0] if single else out_list,
        scratch_shapes=list(scratch),
        compiler_params=pltpu.CompilerParams(vmem_limit_bytes=KERNEL_VMEM),
    )(*args)


def split_heads(qkv_ref, out_ref):
    for h in range(out_ref.shape[0]):
        hd = out_ref.shape[3]
        for j in range(3):
            out_ref[h, j] = qkv_ref[j, :, h * hd : (h + 1) * hd]


def rms_scaled(x):
    return x * lax.rsqrt(jnp.mean(x * x, axis=-1, keepdims=True) + RMS_EPS)


def prepare(arr_ref, rate_ref, q_ref, qn_ref, sent_ref):
    n, _, t, _ = arr_ref.shape
    copies, lines, w = sent_ref.shape
    tok = n * t
    rate = rate_ref[...]
    high = rate.astype(BF16).astype(F32)
    middle = (rate - high).astype(BF16).astype(F32)
    low = rate - high - middle
    spare = jnp.zeros((1, w - 3 * tok), F32)
    rate_rows = jnp.broadcast_to(
        jnp.concatenate([high, middle, low, spare], axis=1), (lines - 2 * tok, w)
    ).astype(BF16)
    for j in range(n):
        rows = slice(j * t, (j + 1) * t)
        q = arr_ref[j, 0]
        q_ref[rows] = q
        qn_ref[rows] = rms_scaled(q.astype(F32)).astype(BF16)
    for d in range(copies):
        for j in range(n):
            sent_ref[d, j * t : (j + 1) * t] = arr_ref[j, 1]
            sent_ref[d, tok + j * t : tok + (j + 1) * t] = arr_ref[j, 2]
        sent_ref[d, 2 * tok :] = rate_rows


def copies_of(rows_ref, out_ref):
    rows = rows_ref[...].astype(BF16)
    for d in range(out_ref.shape[0]):
        out_ref[d] = rows


def merged_rows(ref, m):
    n, _, r, w = ref.shape
    return ref[:, m].astype(F32).reshape(n * r, w)


def gradient(own_ref, other_ref, w_ref, out_ref):
    n, _, r, w = w_ref.shape
    weights = [merged_rows(w_ref, m).astype(BF16) for m in range(3)]
    chips, lines, _ = own_ref.shape
    tok = (lines - RATE_ROWS) // 2
    sums = [None, None, None]
    for ref in (own_ref, other_ref):
        keys = ref[:, :tok].reshape(chips * tok, w)
        values = ref[:, tok : 2 * tok].reshape(chips * tok, w)
        rates = []
        for i in range(chips):
            parts = ref[i, 2 * tok :].astype(F32)[:1]
            rates.append(parts[:, :tok] + parts[:, tok : 2 * tok] + parts[:, 2 * tok : 3 * tok])
        minus_rate = -jnp.concatenate(rates, axis=1)
        key_norm = rms_scaled(keys.astype(F32)).astype(BF16)
        gate = dot_nt(weights[0], key_norm)
        up = dot_nt(weights[1], key_norm)
        back = dot_nt(weights[2], values) * minus_rate
        s = jax.nn.sigmoid(gate)
        silu = gate * s
        lefts = (
            (back * up * s * (1.0 + gate * (1.0 - s)), key_norm),
            (back * silu, key_norm),
            (silu * up * minus_rate, values),
        )
        for m, (left, right) in enumerate(lefts):
            part = dot_nn(left.astype(BF16), right)
            sums[m] = part if sums[m] is None else sums[m] + part
    for m in range(3):
        out_ref[:, m] = sums[m].reshape(n, r, w).astype(BF16)


def sum_and_copy(arr_ref, out_ref):
    total = arr_ref[0].astype(F32)
    for d in range(1, arr_ref.shape[0]):
        total = total + arr_ref[d].astype(F32)
    total = total.astype(BF16)
    for d in range(out_ref.shape[0]):
        out_ref[d] = total


def arrange(where_ref, *refs):
    pieces, out_ref = refs[:-1], refs[-1]
    planes = pieces[0].shape[0]
    for d, piece in enumerate(pieces):
        for z in range(planes):
            out_ref[z * len(pieces) + (where_ref[1] ^ d)] = piece[z]


def attend(where_ref, q_ref, own_ref, other_ref, own_before_ref, other_before_ref, out_ref):
    q = q_ref[...]
    t, w = q.shape
    chips = own_ref.shape[0]
    z, y, core = where_ref[0], where_ref[1], where_ref[2]
    plane = 2 * chips * t
    q_pos = z * plane + (2 * y + core) * t + lax.broadcasted_iota(jnp.int32, (t, chips * t), 0)
    lane = lax.broadcasted_iota(jnp.int32, (t, chips * t), 1)
    lane = lane + lane // t * t
    sides = (
        (own_ref, z, core),
        (other_ref, z, 1 - core),
        (own_before_ref, z - 1, core),
        (other_before_ref, z - 1, 1 - core),
    )
    parts = []
    for ref, k_plane, k_core in sides:
        k_pos = k_plane * plane + k_core * t + lane
        seen = (k_pos <= q_pos) & (k_pos > q_pos - WINDOW) & (k_pos >= 0)
        scores = dot_nt(q, ref[:, :t].reshape(chips * t, w)) * (w ** (-0.5))
        parts.append(jnp.where(seen, scores, -jnp.inf))
    top = jnp.maximum(jnp.maximum(parts[0], parts[1]), jnp.maximum(parts[2], parts[3]))
    top = jnp.max(top, axis=1, keepdims=True)
    parts = [jnp.exp(p - top) for p in parts]
    inverse = 1.0 / jnp.sum(parts[0] + parts[1] + parts[2] + parts[3], axis=1, keepdims=True)
    out = jnp.zeros((t, w), F32)
    for p, (ref, _, _) in zip(parts, sides):
        out = out + dot_nn((p * inverse).astype(BF16), ref[:, t : 2 * t].reshape(chips * t, w))
    out_ref[...] = out


def finish(
    where_ref, rate_ref, g_own, g_other, old_own, old_other, state_ref, qn_ref, att_ref,
    rows_ref, out_ref, x_ref, fresh_ref,
):
    n, _, r, _ = g_own.shape
    half = n * r
    rate = rate_ref[0]
    chip = where_ref[0] * CHIPS_Y + where_ref[1]

    xs = []
    for m in range(3):
        g = jnp.concatenate([merged_rows(g_own, m), merged_rows(g_other, m)], axis=0)
        xs.append(g / (jnp.sqrt(jnp.sum(g * g, keepdims=True)) + NORM_EPS))
    for _ in range(NS_STEPS):
        lows = [x.astype(BF16) for x in xs]
        grams = [dot_nt(low, low) for low in lows]
        gram_lows = [gram.astype(BF16) for gram in grams]
        squares = [dot_nn(gram, gram) for gram in gram_lows]
        polys = [(NS_2 * gram + NS_3 * sq).astype(BF16) for gram, sq in zip(grams, squares)]
        moved = [dot_nn(poly, low) for poly, low in zip(polys, lows)]
        xs = [NS_1 * x + move for x, move in zip(xs, moved)]
    for m, x in enumerate(xs):
        fresh_ref[m, :half] = (merged_rows(old_own, m) - rate * x[:half]).astype(BF16)
        fresh_ref[m, half:] = (merged_rows(old_other, m) - rate * x[half:]).astype(BF16)
        x_ref[m] = x[:half]
        rows_ref[m] = state_ref[m] - rate * x_ref[m, pl.ds(pl.multiple_of(chip * r, r), r)]
    gate = dot_nt(qn_ref[...], fresh_ref[0])
    up = dot_nt(qn_ref[...], fresh_ref[1])
    active = (jax.nn.silu(gate) * up).astype(BF16)
    out_ref[...] = (att_ref[...] + dot_nn(active, fresh_ref[2])).astype(BF16)


def join_heads(arr_ref, out_ref):
    for h in range(arr_ref.shape[0]):
        hd = arr_ref.shape[2]
        out_ref[:, h * hd : (h + 1) * hd] = arr_ref[h]


def shards(qkv, token_rate, head_rate, fast_state):
    heads = lax.axis_size("head")
    chips = CHIPS_Z * CHIPS_Y
    _, tok_part, width = qkv.shape
    hd = width // heads
    tok = tok_part * heads
    rows = fast_state.shape[2]
    where = jnp.stack([lax.axis_index(a) for a in SEQ]).astype(jnp.int32)
    state = fast_state[:, 0]
    swap = [(0, 1), (1, 0)]

    def shape(dims, dtype=BF16):
        return jax.ShapeDtypeStruct(dims, dtype)

    def exchanged(pieces, axis):
        return lax.all_to_all(pieces, axis, 0, 0, tiled=True)

    split = local_call(
        split_heads, shape((heads, 3, tok_part, hd)), (qkv,), hbm_in=(0,), hbm_out=(0,)
    )
    arrived = exchanged(split, "head")
    old_copies = local_call(copies_of, shape((CHIPS_Z, 3, rows, hd)), (state,), hbm_out=(0,))
    old_slice = exchanged(old_copies, "z")
    q, q_norm, sent = local_call(
        prepare,
        [shape((tok, hd)), shape((tok, hd)), shape((CHIPS_Y, 2 * tok + RATE_ROWS, hd))],
        (arrived, token_rate.reshape(1, tok)),
        hbm_out=(2,),
    )
    kv_own = exchanged(sent, "y")
    kv_other = lax.ppermute(kv_own, "core", swap)
    partial = local_call(
        gradient, shape((CHIPS_Z, 3, rows, hd)), (kv_own, kv_other, old_slice), hbm_out=(0,)
    )
    parts = exchanged(partial, "z")
    g_copies = local_call(sum_and_copy, shape((chips, 3, rows, hd)), (parts,), hbm_out=(0,))
    g_own = exchanged(g_copies, CHIPS)
    ring = [(i, (i + 1) % CHIPS_Z) for i in range(CHIPS_Z)]
    kv_own_before = lax.ppermute(kv_own, "z", ring)
    kv_other_before = lax.ppermute(kv_own_before, "core", swap)
    attention = local_call(
        attend,
        shape((tok, hd), F32),
        (where, q, kv_own, kv_other, kv_own_before, kv_other_before),
        smem=(0,),
    )
    olds = [old_slice] + [
        lax.ppermute(old_slice, "y", [(i, i ^ d) for i in range(CHIPS_Y)])
        for d in range(1, CHIPS_Y)
    ]
    old_own = local_call(arrange, shape((chips, 3, rows, hd)), (where, *olds), smem=(0,))
    old_other = lax.ppermute(old_own, "core", swap)
    g_other = lax.ppermute(g_own, "core", swap)
    new_rows, combined = local_call(
        finish,
        [shape((3, rows, hd), F32), shape((tok, hd))],
        (where, head_rate, g_own, g_other, old_own, old_other, state, q_norm, attention),
        smem=(0, 1),
        hbm_out=(0, 1),
        scratch=[
            pltpu.VMEM((3, chips * rows, hd), F32),
            pltpu.VMEM((3, 2 * chips * rows, hd), BF16),
        ],
    )
    back = exchanged(combined.reshape(heads, tok_part, hd), "head")
    return (
        local_call(join_heads, shape((tok_part, width)), (back,), hbm_out=(0,)),
        new_rows[:, None],
    )


def solution(mesh):
    finer = Mesh(mesh.devices.reshape(CHIPS_Z, CHIPS_Y, 2, mesh.shape["head"]), SEQ_HEAD)
    return jax.shard_map(
        shards,
        mesh=finer,
        in_specs=(P(None, SEQ_HEAD, None), P(SEQ, "head"), P("head"), P(None, "head", SEQ, None)),
        out_specs=(P(SEQ_HEAD, None), P(None, "head", SEQ, None)),
        check_vma=False,
    )
```

```python
import jax
import jax.numpy as jnp
from jax import lax
from jax.experimental import pallas as pl
from jax.experimental.pallas import tpu as pltpu
from jax.sharding import Mesh
from jax.sharding import PartitionSpec as P

WINDOW = 1024
NS_STEPS = 2
NS_1, NS_2, NS_3 = 3.4445, -4.775, 2.0315
RMS_EPS = 1e-06
NORM_EPS = 1e-07

SEQ = ("z", "y", "core")
SEQ_HEAD = ("z", "y", "core", "head")
CHIPS = ("z", "y")
F32, BF16 = jnp.float32, jnp.bfloat16
CHIPS_Z, CHIPS_Y = 8, 4
RATE_ROWS = 8
KERNEL_VMEM = 20 * 1024 * 1024


def dot_nt(a, b):
    return lax.dot_general(a, b, (((1,), (1,)), ((), ())), preferred_element_type=F32)


def dot_nn(a, b):
    return lax.dot_general(a, b, (((1,), (0,)), ((), ())), preferred_element_type=F32)


def local_call(body, outs, args, smem=(), scratch=(), hbm_in=(), hbm_out=()):
    specs = [
        pl.BlockSpec(memory_space=pltpu.SMEM if i in smem else pltpu.VMEM) for i in range(len(args))
    ]
    single = not isinstance(outs, (list, tuple))
    out_list = [outs] if single else list(outs)
    out_list = [
        (pltpu.HBM if i in hbm_out else pltpu.VMEM)(o.shape, o.dtype)
        for i, o in enumerate(out_list)
    ]
    args = [
        a if i in smem or i in hbm_in else pltpu.with_memory_space_constraint(a, pltpu.VMEM)
        for i, a in enumerate(args)
    ]
    out_specs = [pl.BlockSpec(memory_space=pltpu.VMEM) for _ in out_list]
    return pl.pallas_call(
        body,
        in_specs=specs,
        out_specs=out_specs[0] if single else out_specs,
        out_shape=out_list[0] if single else out_list,
        scratch_shapes=list(scratch),
        compiler_params=pltpu.CompilerParams(vmem_limit_bytes=KERNEL_VMEM),
    )(*args)


def split_heads(qkv_ref, out_ref):
    for h in range(out_ref.shape[0]):
        hd = out_ref.shape[3]
        for j in range(3):
            out_ref[h, j] = qkv_ref[j, :, h * hd : (h + 1) * hd]


def rms_scaled(x):
    return x * lax.rsqrt(jnp.mean(x * x, axis=-1, keepdims=True) + RMS_EPS)


def prepare(arr_ref, rate_ref, q_ref, qn_ref, sent_ref):
    n, _, t, _ = arr_ref.shape
    lines, w = sent_ref.shape
    tok = n * t
    rate = rate_ref[...]
    high = rate.astype(BF16).astype(F32)
    middle = (rate - high).astype(BF16).astype(F32)
    low = rate - high - middle
    spare = jnp.zeros((1, w - 3 * tok), F32)
    rate_rows = jnp.broadcast_to(
        jnp.concatenate([high, middle, low, spare], axis=1), (lines - 2 * tok, w)
    ).astype(BF16)
    for j in range(n):
        rows = slice(j * t, (j + 1) * t)
        q = arr_ref[j, 0]
        q_ref[rows] = q
        qn_ref[rows] = rms_scaled(q.astype(F32)).astype(BF16)
    for j in range(n):
        sent_ref[j * t : (j + 1) * t] = arr_ref[j, 1]
        sent_ref[tok + j * t : tok + (j + 1) * t] = arr_ref[j, 2]
    sent_ref[2 * tok :] = rate_rows


def old_copies(where_ref, near_ref, far_ref, out_ref):
    for z in range(out_ref.shape[0]):
        for ref, odd in ((near_ref, 0), (far_ref, 1)):
            for i in range(2):
                out_ref[z, where_ref[1] ^ (2 * i + odd)] = ref[i]


def in_order(where_ref, *refs):
    pieces, out_ref = refs[:-1], refs[-1]
    for d, piece in enumerate(pieces):
        out_ref[(where_ref[1] + CHIPS_Y - d) % CHIPS_Y] = piece[...]


def merged_rows(ref, m):
    n, _, r, w = ref.shape
    return ref[:, m].astype(F32).reshape(n * r, w)


def gradient(where_ref, own_ref, other_ref, w_ref, out_ref):
    n, _, r, w = out_ref.shape
    weights = []
    for m in range(3):
        rows = [w_ref[z * CHIPS_Y + where_ref[1], m].astype(F32) for z in range(n)]
        weights.append(jnp.concatenate(rows, axis=0).astype(BF16))
    chips, lines, _ = own_ref.shape
    tok = (lines - RATE_ROWS) // 2
    sums = [None, None, None]
    for ref in (own_ref, other_ref):
        keys = ref[:, :tok].reshape(chips * tok, w)
        values = ref[:, tok : 2 * tok].reshape(chips * tok, w)
        rates = []
        for i in range(chips):
            parts = ref[i, 2 * tok :].astype(F32)[:1]
            rates.append(parts[:, :tok] + parts[:, tok : 2 * tok] + parts[:, 2 * tok : 3 * tok])
        minus_rate = -jnp.concatenate(rates, axis=1)
        key_norm = rms_scaled(keys.astype(F32)).astype(BF16)
        gate = dot_nt(weights[0], key_norm)
        up = dot_nt(weights[1], key_norm)
        back = dot_nt(weights[2], values) * minus_rate
        s = jax.nn.sigmoid(gate)
        silu = gate * s
        lefts = (
            (back * up * s * (1.0 + gate * (1.0 - s)), key_norm),
            (back * silu, key_norm),
            (silu * up * minus_rate, values),
        )
        for m, (left, right) in enumerate(lefts):
            part = dot_nn(left.astype(BF16), right)
            sums[m] = part if sums[m] is None else sums[m] + part
    for m in range(3):
        out_ref[:, m] = sums[m].reshape(n, r, w).astype(BF16)


def sum_and_copy(arr_ref, out_ref):
    total = arr_ref[0].astype(F32)
    for d in range(1, arr_ref.shape[0]):
        total = total + arr_ref[d].astype(F32)
    total = total.astype(BF16)
    for d in range(out_ref.shape[0]):
        out_ref[d] = total


def attend(where_ref, q_ref, own_ref, other_ref, own_before_ref, other_before_ref, out_ref):
    q = q_ref[...]
    t, w = q.shape
    chips = own_ref.shape[0]
    z, y, core = where_ref[0], where_ref[1], where_ref[2]
    plane = 2 * chips * t
    q_pos = z * plane + (2 * y + core) * t + lax.broadcasted_iota(jnp.int32, (t, chips * t), 0)
    lane = lax.broadcasted_iota(jnp.int32, (t, chips * t), 1)
    lane = lane + lane // t * t
    sides = (
        (own_ref, z, core),
        (other_ref, z, 1 - core),
        (own_before_ref, z - 1, core),
        (other_before_ref, z - 1, 1 - core),
    )
    parts = []
    for ref, k_plane, k_core in sides:
        k_pos = k_plane * plane + k_core * t + lane
        seen = (k_pos <= q_pos) & (k_pos > q_pos - WINDOW) & (k_pos >= 0)
        scores = dot_nt(q, ref[:, :t].reshape(chips * t, w)) * (w ** (-0.5))
        parts.append(jnp.where(seen, scores, -jnp.inf))
    top = jnp.maximum(jnp.maximum(parts[0], parts[1]), jnp.maximum(parts[2], parts[3]))
    top = jnp.max(top, axis=1, keepdims=True)
    parts = [jnp.exp(p - top) for p in parts]
    inverse = 1.0 / jnp.sum(parts[0] + parts[1] + parts[2] + parts[3], axis=1, keepdims=True)
    out = jnp.zeros((t, w), F32)
    for p, (ref, _, _) in zip(parts, sides):
        out = out + dot_nn((p * inverse).astype(BF16), ref[:, t : 2 * t].reshape(chips * t, w))
    out_ref[...] = out


def finish(
    where_ref, rate_ref, g_own, g_other, old_own, old_other, state_ref, qn_ref, att_ref,
    rows_ref, out_ref, x_ref, fresh_ref,
):
    n, _, r, _ = g_own.shape
    half = n * r
    rate = rate_ref[0]
    chip = where_ref[0] * CHIPS_Y + where_ref[1]

    xs = []
    for m in range(3):
        g = jnp.concatenate([merged_rows(g_own, m), merged_rows(g_other, m)], axis=0)
        xs.append(g / (jnp.sqrt(jnp.sum(g * g, keepdims=True)) + NORM_EPS))
    for _ in range(NS_STEPS):
        lows = [x.astype(BF16) for x in xs]
        grams = [dot_nt(low, low) for low in lows]
        gram_lows = [gram.astype(BF16) for gram in grams]
        squares = [dot_nn(gram, gram) for gram in gram_lows]
        polys = [(NS_2 * gram + NS_3 * sq).astype(BF16) for gram, sq in zip(grams, squares)]
        moved = [dot_nn(poly, low) for poly, low in zip(polys, lows)]
        xs = [NS_1 * x + move for x, move in zip(xs, moved)]
    for m, x in enumerate(xs):
        fresh_ref[m, :half] = (merged_rows(old_own, m) - rate * x[:half]).astype(BF16)
        fresh_ref[m, half:] = (merged_rows(old_other, m) - rate * x[half:]).astype(BF16)
        x_ref[m] = x[:half]
        rows_ref[m] = state_ref[m] - rate * x_ref[m, pl.ds(pl.multiple_of(chip * r, r), r)]
    gate = dot_nt(qn_ref[...], fresh_ref[0])
    up = dot_nt(qn_ref[...], fresh_ref[1])
    active = (jax.nn.silu(gate) * up).astype(BF16)
    out_ref[...] = (att_ref[...] + dot_nn(active, fresh_ref[2])).astype(BF16)


def join_heads(arr_ref, out_ref):
    for h in range(arr_ref.shape[0]):
        hd = arr_ref.shape[2]
        out_ref[:, h * hd : (h + 1) * hd] = arr_ref[h]


def shards(qkv, token_rate, head_rate, fast_state):
    heads = lax.axis_size("head")
    chips = CHIPS_Z * CHIPS_Y
    _, tok_part, width = qkv.shape
    hd = width // heads
    tok = tok_part * heads
    rows = fast_state.shape[2]
    where = jnp.stack([lax.axis_index(a) for a in SEQ]).astype(jnp.int32)
    state = fast_state[:, 0]
    swap = [(0, 1), (1, 0)]

    def shape(dims, dtype=BF16):
        return jax.ShapeDtypeStruct(dims, dtype)

    def exchanged(pieces, axis):
        return lax.all_to_all(pieces, axis, 0, 0, tiled=True)

    split = local_call(
        split_heads, shape((heads, 3, tok_part, hd)), (qkv,), hbm_in=(0,), hbm_out=(0,)
    )
    arrived = exchanged(split, "head")

    def across(distance):
        return [(i, i ^ distance) for i in range(CHIPS_Y)]

    old_one = state.astype(BF16)[None]
    old_two = jnp.concatenate([old_one, lax.ppermute(old_one, "y", across(2))])
    old_far = lax.ppermute(old_two, "y", across(1))
    copies = local_call(
        old_copies,
        shape((CHIPS_Z, CHIPS_Y, 3, rows, hd)),
        (where, old_two, old_far),
        smem=(0,),
        hbm_out=(0,),
    )
    old_own = exchanged(copies, "z").reshape(chips, 3, rows, hd)
    q, q_norm, sent = local_call(
        prepare,
        [shape((tok, hd)), shape((tok, hd)), shape((2 * tok + RATE_ROWS, hd))],
        (arrived, token_rate.reshape(1, tok)),
        hbm_out=(0, 1),
    )

    def behind(distance):
        return [(i, (i + distance) % CHIPS_Y) for i in range(CHIPS_Y)]

    relay = [(2 * i, 2 * j) for i, j in behind(1)] + [(2 * i + 1, 2 * j + 1) for i, j in behind(3)]

    def of_plane(block):
        one = lax.ppermute(block, "y", behind(1))
        three = lax.ppermute(block, "y", behind(3))
        relayed = jnp.where(lax.axis_index("core") == 0, one, three)
        two = lax.ppermute(relayed, ("y", "core"), relay)
        return local_call(
            in_order,
            shape((CHIPS_Y, *block.shape)),
            (where, block, one, two, three),
            smem=(0,),
        )

    kv_own = of_plane(sent)
    kv_other = lax.ppermute(kv_own, "core", swap)
    partial = local_call(
        gradient,
        shape((CHIPS_Z, 3, rows, hd)),
        (where, kv_own, kv_other, old_own),
        smem=(0,),
        hbm_out=(0,),
    )
    parts = exchanged(partial, "z")
    g_copies = local_call(sum_and_copy, shape((chips, 3, rows, hd)), (parts,), hbm_out=(0,))
    g_own = exchanged(g_copies, CHIPS)
    ring = [(i, (i + 1) % CHIPS_Z) for i in range(CHIPS_Z)]
    kv_own_before = of_plane(lax.ppermute(sent, "z", ring))
    kv_other_before = lax.ppermute(kv_own_before, "core", swap)
    attention = local_call(
        attend,
        shape((tok, hd), F32),
        (where, q, kv_own, kv_other, kv_own_before, kv_other_before),
        smem=(0,),
        hbm_in=(1,),
    )
    old_other = lax.ppermute(old_own, "core", swap)
    g_other = lax.ppermute(g_own, "core", swap)
    new_rows, combined = local_call(
        finish,
        [shape((3, rows, hd), F32), shape((tok, hd))],
        (where, head_rate, g_own, g_other, old_own, old_other, state, q_norm, attention),
        smem=(0, 1),
        hbm_in=(6, 7),
        hbm_out=(0, 1),
        scratch=[
            pltpu.VMEM((3, chips * rows, hd), F32),
            pltpu.VMEM((3, 2 * chips * rows, hd), BF16),
        ],
    )
    back = exchanged(combined.reshape(heads, tok_part, hd), "head")
    return (
        local_call(join_heads, shape((tok_part, width)), (back,), hbm_out=(0,)),
        new_rows[:, None],
    )


def solution(mesh):
    finer = Mesh(mesh.devices.reshape(CHIPS_Z, CHIPS_Y, 2, mesh.shape["head"]), SEQ_HEAD)
    return jax.shard_map(
        shards,
        mesh=finer,
        in_specs=(P(None, SEQ_HEAD, None), P(SEQ, "head"), P("head"), P(None, "head", SEQ, None)),
        out_specs=(P(SEQ_HEAD, None), P(None, "head", SEQ, None)),
        check_vma=False,
    )
```

```python
import jax
import jax.numpy as jnp
from jax import lax
from jax.experimental import pallas as pl
from jax.experimental.pallas import tpu as pltpu
from jax.sharding import Mesh
from jax.sharding import PartitionSpec as P

WINDOW = 1024
NS_STEPS = 2
NS_1, NS_2, NS_3 = 3.4445, -4.775, 2.0315
RMS_EPS = 1e-06
NORM_EPS = 1e-07

SEQ = ("z", "y", "core")
SEQ_HEAD = ("z", "y", "core", "head")
CHIPS = ("z", "y")
F32, BF16 = jnp.float32, jnp.bfloat16
CHIPS_Z, CHIPS_Y = 8, 4
RATE_ROWS = 8
KERNEL_VMEM = 20 * 1024 * 1024


def dot_nt(a, b):
    return lax.dot_general(a, b, (((1,), (1,)), ((), ())), preferred_element_type=F32)


def dot_nn(a, b):
    return lax.dot_general(a, b, (((1,), (0,)), ((), ())), preferred_element_type=F32)


def local_call(body, outs, args, smem=(), scratch=(), hbm_in=(), hbm_out=()):
    specs = [
        pl.BlockSpec(memory_space=pltpu.SMEM if i in smem else pltpu.VMEM) for i in range(len(args))
    ]
    single = not isinstance(outs, (list, tuple))
    out_list = [outs] if single else list(outs)
    out_list = [
        (pltpu.HBM if i in hbm_out else pltpu.VMEM)(o.shape, o.dtype)
        for i, o in enumerate(out_list)
    ]
    args = [
        a if i in smem or i in hbm_in else pltpu.with_memory_space_constraint(a, pltpu.VMEM)
        for i, a in enumerate(args)
    ]
    out_specs = [pl.BlockSpec(memory_space=pltpu.VMEM) for _ in out_list]
    return pl.pallas_call(
        body,
        in_specs=specs,
        out_specs=out_specs[0] if single else out_specs,
        out_shape=out_list[0] if single else out_list,
        scratch_shapes=list(scratch),
        compiler_params=pltpu.CompilerParams(vmem_limit_bytes=KERNEL_VMEM),
    )(*args)


def split_heads(qkv_ref, out_ref):
    for h in range(out_ref.shape[0]):
        hd = out_ref.shape[3]
        for j in range(3):
            out_ref[h, j] = qkv_ref[j, :, h * hd : (h + 1) * hd]


def rms_scaled(x):
    return x * lax.rsqrt(jnp.mean(x * x, axis=-1, keepdims=True) + RMS_EPS)


def prepare(arr_ref, rate_ref, q_ref, qn_ref, sent_ref):
    n, _, t, _ = arr_ref.shape
    copies, lines, w = sent_ref.shape
    tok = n * t
    rate = rate_ref[...]
    high = rate.astype(BF16).astype(F32)
    middle = (rate - high).astype(BF16).astype(F32)
    low = rate - high - middle
    spare = jnp.zeros((1, w - 3 * tok), F32)
    rate_rows = jnp.broadcast_to(
        jnp.concatenate([high, middle, low, spare], axis=1), (lines - 2 * tok, w)
    ).astype(BF16)
    for j in range(n):
        rows = slice(j * t, (j + 1) * t)
        q = arr_ref[j, 0]
        q_ref[rows] = q
        qn_ref[rows] = rms_scaled(q.astype(F32)).astype(BF16)
    for d in range(copies):
        for j in range(n):
            sent_ref[d, j * t : (j + 1) * t] = arr_ref[j, 1]
            sent_ref[d, tok + j * t : tok + (j + 1) * t] = arr_ref[j, 2]
        sent_ref[d, 2 * tok :] = rate_rows


def merged_rows(ref, m):
    n, _, r, w = ref.shape
    return ref[:, m].astype(F32).reshape(n * r, w)


def gradient(own_ref, other_ref, w_ref, out_ref):
    n, _, r, w = w_ref.shape
    weights = [merged_rows(w_ref, m).astype(BF16) for m in range(3)]
    chips, lines, _ = own_ref.shape
    tok = (lines - RATE_ROWS) // 2
    sums = [None, None, None]
    for ref in (own_ref, other_ref):
        keys = ref[:, :tok].reshape(chips * tok, w)
        values = ref[:, tok : 2 * tok].reshape(chips * tok, w)
        rates = []
        for i in range(chips):
            parts = ref[i, 2 * tok :].astype(F32)[:1]
            rates.append(parts[:, :tok] + parts[:, tok : 2 * tok] + parts[:, 2 * tok : 3 * tok])
        minus_rate = -jnp.concatenate(rates, axis=1)
        key_norm = rms_scaled(keys.astype(F32)).astype(BF16)
        gate = dot_nt(weights[0], key_norm)
        up = dot_nt(weights[1], key_norm)
        back = dot_nt(weights[2], values) * minus_rate
        s = jax.nn.sigmoid(gate)
        silu = gate * s
        lefts = (
            (back * up * s * (1.0 + gate * (1.0 - s)), key_norm),
            (back * silu, key_norm),
            (silu * up * minus_rate, values),
        )
        for m, (left, right) in enumerate(lefts):
            part = dot_nn(left.astype(BF16), right)
            sums[m] = part if sums[m] is None else sums[m] + part
    for m in range(3):
        out_ref[:, m] = sums[m].reshape(n, r, w).astype(BF16)


def sum_and_copy(arr_ref, out_ref):
    total = arr_ref[0].astype(F32)
    for d in range(1, arr_ref.shape[0]):
        total = total + arr_ref[d].astype(F32)
    total = total.astype(BF16)
    for d in range(out_ref.shape[0]):
        out_ref[d] = total


def slice_of(where_ref, near_ref, far_ref, out_ref):
    for ref, odd in ((near_ref, 0), (far_ref, 1)):
        for i, d in enumerate((0, 4, 2, 6)):
            out_ref[where_ref[0] ^ (d + odd)] = ref[i]


def arrange(where_ref, *refs):
    pieces, out_ref = refs[:-1], refs[-1]
    planes = pieces[0].shape[0]
    for d, piece in enumerate(pieces):
        for z in range(planes):
            out_ref[z * len(pieces) + (where_ref[1] ^ d)] = piece[z]


def attend(where_ref, q_ref, own_ref, other_ref, own_before_ref, other_before_ref, out_ref):
    q = q_ref[...]
    t, w = q.shape
    chips = own_ref.shape[0]
    z, y, core = where_ref[0], where_ref[1], where_ref[2]
    plane = 2 * chips * t
    q_pos = z * plane + (2 * y + core) * t + lax.broadcasted_iota(jnp.int32, (t, chips * t), 0)
    lane = lax.broadcasted_iota(jnp.int32, (t, chips * t), 1)
    lane = lane + lane // t * t
    sides = (
        (own_ref, z, core),
        (other_ref, z, 1 - core),
        (own_before_ref, z - 1, core),
        (other_before_ref, z - 1, 1 - core),
    )
    parts = []
    for ref, k_plane, k_core in sides:
        k_pos = k_plane * plane + k_core * t + lane
        seen = (k_pos <= q_pos) & (k_pos > q_pos - WINDOW) & (k_pos >= 0)
        scores = dot_nt(q, ref[:, :t].reshape(chips * t, w)) * (w ** (-0.5))
        parts.append(jnp.where(seen, scores, -jnp.inf))
    top = jnp.maximum(jnp.maximum(parts[0], parts[1]), jnp.maximum(parts[2], parts[3]))
    top = jnp.max(top, axis=1, keepdims=True)
    parts = [jnp.exp(p - top) for p in parts]
    inverse = 1.0 / jnp.sum(parts[0] + parts[1] + parts[2] + parts[3], axis=1, keepdims=True)
    out = jnp.zeros((t, w), F32)
    for p, (ref, _, _) in zip(parts, sides):
        out = out + dot_nn((p * inverse).astype(BF16), ref[:, t : 2 * t].reshape(chips * t, w))
    out_ref[...] = out


def finish(
    where_ref, rate_ref, g_own, g_other, old_own, old_other, state_ref, qn_ref, att_ref,
    rows_ref, out_ref, x_ref, fresh_ref,
):
    n, _, r, _ = g_own.shape
    half = n * r
    rate = rate_ref[0]
    chip = where_ref[0] * CHIPS_Y + where_ref[1]

    xs = []
    for m in range(3):
        g = jnp.concatenate([merged_rows(g_own, m), merged_rows(g_other, m)], axis=0)
        xs.append(g / (jnp.sqrt(jnp.sum(g * g, keepdims=True)) + NORM_EPS))
    for _ in range(NS_STEPS):
        lows = [x.astype(BF16) for x in xs]
        grams = [dot_nt(low, low) for low in lows]
        gram_lows = [gram.astype(BF16) for gram in grams]
        squares = [dot_nn(gram, gram) for gram in gram_lows]
        polys = [(NS_2 * gram + NS_3 * sq).astype(BF16) for gram, sq in zip(grams, squares)]
        moved = [dot_nn(poly, low) for poly, low in zip(polys, lows)]
        xs = [NS_1 * x + move for x, move in zip(xs, moved)]
    for m, x in enumerate(xs):
        fresh_ref[m, :half] = (merged_rows(old_own, m) - rate * x[:half]).astype(BF16)
        fresh_ref[m, half:] = (merged_rows(old_other, m) - rate * x[half:]).astype(BF16)
        x_ref[m] = x[:half]
        rows_ref[m] = state_ref[m] - rate * x_ref[m, pl.ds(pl.multiple_of(chip * r, r), r)]
    gate = dot_nt(qn_ref[...], fresh_ref[0])
    up = dot_nt(qn_ref[...], fresh_ref[1])
    active = (jax.nn.silu(gate) * up).astype(BF16)
    out_ref[...] = (att_ref[...] + dot_nn(active, fresh_ref[2])).astype(BF16)


def join_heads(arr_ref, out_ref):
    for h in range(arr_ref.shape[0]):
        hd = arr_ref.shape[2]
        out_ref[:, h * hd : (h + 1) * hd] = arr_ref[h]


def shards(qkv, token_rate, head_rate, fast_state):
    heads = lax.axis_size("head")
    chips = CHIPS_Z * CHIPS_Y
    _, tok_part, width = qkv.shape
    hd = width // heads
    tok = tok_part * heads
    rows = fast_state.shape[2]
    where = jnp.stack([lax.axis_index(a) for a in SEQ]).astype(jnp.int32)
    state = fast_state[:, 0]
    swap = [(0, 1), (1, 0)]

    def shape(dims, dtype=BF16):
        return jax.ShapeDtypeStruct(dims, dtype)

    def exchanged(pieces, axis):
        return lax.all_to_all(pieces, axis, 0, 0, tiled=True)

    split = local_call(
        split_heads, shape((heads, 3, tok_part, hd)), (qkv,), hbm_in=(0,), hbm_out=(0,)
    )
    arrived = exchanged(split, "head")
    q, q_norm, sent = local_call(
        prepare,
        [shape((tok, hd)), shape((tok, hd)), shape((CHIPS_Y, 2 * tok + RATE_ROWS, hd))],
        (arrived, token_rate.reshape(1, tok)),
        hbm_out=(0, 1, 2),
    )
    kv_own = exchanged(sent, "y")

    def across(distance):
        return [(i, i ^ distance) for i in range(CHIPS_Z)]

    old_two = state.astype(BF16)[None]
    old_two = jnp.concatenate([old_two, lax.ppermute(old_two, "z", across(4))])
    old_four = jnp.concatenate([old_two, lax.ppermute(old_two, "z", across(2))])
    old_far = lax.ppermute(old_four, "z", across(1))
    old_slice = local_call(
        slice_of, shape((CHIPS_Z, 3, rows, hd)), (where, old_four, old_far), smem=(0,)
    )
    kv_other = lax.ppermute(kv_own, "core", swap)
    partial = local_call(
        gradient, shape((CHIPS_Z, 3, rows, hd)), (kv_own, kv_other, old_slice), hbm_out=(0,)
    )
    parts = exchanged(partial, "z")
    g_copies = local_call(sum_and_copy, shape((chips, 3, rows, hd)), (parts,), hbm_out=(0,))
    g_own = exchanged(g_copies, CHIPS)
    ring = [(i, (i + 1) % CHIPS_Z) for i in range(CHIPS_Z)]
    kv_own_before = lax.ppermute(kv_own, "z", ring)
    kv_other_before = lax.ppermute(kv_own_before, "core", swap)
    attention = local_call(
        attend,
        shape((tok, hd), F32),
        (where, q, kv_own, kv_other, kv_own_before, kv_other_before),
        smem=(0,),
    )
    olds = [old_slice] + [
        lax.ppermute(old_slice, "y", [(i, i ^ d) for i in range(CHIPS_Y)])
        for d in range(1, CHIPS_Y)
    ]
    old_own = local_call(arrange, shape((chips, 3, rows, hd)), (where, *olds), smem=(0,))
    old_other = lax.ppermute(old_own, "core", swap)
    g_other = lax.ppermute(g_own, "core", swap)
    new_rows, combined = local_call(
        finish,
        [shape((3, rows, hd), F32), shape((tok, hd))],
        (where, head_rate, g_own, g_other, old_own, old_other, state, q_norm, attention),
        smem=(0, 1),
        hbm_out=(0, 1),
        scratch=[
            pltpu.VMEM((3, chips * rows, hd), F32),
            pltpu.VMEM((3, 2 * chips * rows, hd), BF16),
        ],
    )
    back = exchanged(combined.reshape(heads, tok_part, hd), "head")
    return (
        local_call(join_heads, shape((tok_part, width)), (back,), hbm_out=(0,)),
        new_rows[:, None],
    )


def solution(mesh):
    finer = Mesh(mesh.devices.reshape(CHIPS_Z, CHIPS_Y, 2, mesh.shape["head"]), SEQ_HEAD)
    return jax.shard_map(
        shards,
        mesh=finer,
        in_specs=(P(None, SEQ_HEAD, None), P(SEQ, "head"), P("head"), P(None, "head", SEQ, None)),
        out_specs=(P(SEQ_HEAD, None), P(None, "head", SEQ, None)),
        check_vma=False,
    )
```

```python
import jax
import jax.numpy as jnp
from jax import lax
from jax.experimental import pallas as pl
from jax.experimental.pallas import tpu as pltpu
from jax.sharding import Mesh
from jax.sharding import PartitionSpec as P

WINDOW = 1024
NS_STEPS = 2
NS_1, NS_2, NS_3 = 3.4445, -4.775, 2.0315
RMS_EPS = 1e-06
NORM_EPS = 1e-07
HIDDEN = -1e30

SEQ = ("z", "y", "core")
SEQ_HEAD = ("z", "y", "core", "head")
CHIPS = ("z", "y")
F32, BF16 = jnp.float32, jnp.bfloat16
CHIPS_Z, CHIPS_Y = 8, 4
RATE_ROWS = 8
KERNEL_VMEM = 18 * 1024 * 1024


def dot_nt(a, b):
    return lax.dot_general(a, b, (((1,), (1,)), ((), ())), preferred_element_type=F32)


def dot_nn(a, b):
    return lax.dot_general(a, b, (((1,), (0,)), ((), ())), preferred_element_type=F32)


def local_call(body, outs, args, smem=(), scratch=(), hbm_in=(), hbm_out=()):
    specs = [
        pl.BlockSpec(memory_space=pltpu.SMEM if i in smem else pltpu.VMEM) for i in range(len(args))
    ]
    single = not isinstance(outs, (list, tuple))
    out_list = [outs] if single else list(outs)
    out_list = [
        (pltpu.HBM if i in hbm_out else pltpu.VMEM)(o.shape, o.dtype)
        for i, o in enumerate(out_list)
    ]
    args = [
        a if i in smem or i in hbm_in else pltpu.with_memory_space_constraint(a, pltpu.VMEM)
        for i, a in enumerate(args)
    ]
    out_specs = [pl.BlockSpec(memory_space=pltpu.VMEM) for _ in out_list]
    return pl.pallas_call(
        body,
        in_specs=specs,
        out_specs=out_specs[0] if single else out_specs,
        out_shape=out_list[0] if single else out_list,
        scratch_shapes=list(scratch),
        compiler_params=pltpu.CompilerParams(vmem_limit_bytes=KERNEL_VMEM),
    )(*args)


def split_heads(qkv_ref, out_ref):
    for h in range(out_ref.shape[0]):
        hd = out_ref.shape[3]
        for j in range(3):
            out_ref[h, j] = qkv_ref[j, :, h * hd : (h + 1) * hd]


def rms_scaled(x):
    return x * lax.rsqrt(jnp.mean(x * x, axis=-1, keepdims=True) + RMS_EPS)


def prepare(arr_ref, rate_ref, q_ref, qn_ref, sent_ref):
    n, _, t, _ = arr_ref.shape
    copies, lines, w = sent_ref.shape
    tok = n * t
    rate = rate_ref[...]
    high, middle, low = in_parts(rate)
    spare = jnp.zeros((1, w - 3 * tok), F32)
    rate_rows = jnp.broadcast_to(
        jnp.concatenate([high, middle, low, spare], axis=1), (lines - 2 * tok, w)
    ).astype(BF16)
    for j in range(n):
        rows = slice(j * t, (j + 1) * t)
        q = arr_ref[j, 0]
        q_ref[rows] = q
        qn_ref[rows] = rms_scaled(q.astype(F32)).astype(BF16)
    for d in range(copies):
        for j in range(n):
            sent_ref[d, j * t : (j + 1) * t] = arr_ref[j, 1]
            sent_ref[d, tok + j * t : tok + (j + 1) * t] = arr_ref[j, 2]
        sent_ref[d, 2 * tok :] = rate_rows


def merged_rows(ref, m):
    n, _, r, w = ref.shape
    return ref[:, m].astype(F32).reshape(n * r, w)


def gradient(own_ref, other_ref, w_ref, out_ref):
    n, _, r, w = w_ref.shape
    weights = [merged_rows(w_ref, m).astype(BF16) for m in range(3)]
    chips, lines, _ = own_ref.shape
    tok = (lines - RATE_ROWS) // 2
    sums = [None, None, None]
    for ref in (own_ref, other_ref):
        keys = ref[:, :tok].reshape(chips * tok, w)
        values = ref[:, tok : 2 * tok].reshape(chips * tok, w)
        rates = []
        for i in range(chips):
            parts = ref[i, 2 * tok :].astype(F32)[:1]
            rates.append(parts[:, :tok] + parts[:, tok : 2 * tok] + parts[:, 2 * tok : 3 * tok])
        minus_rate = -jnp.concatenate(rates, axis=1)
        key_norm = rms_scaled(keys.astype(F32)).astype(BF16)
        gate = dot_nt(weights[0], key_norm)
        up = dot_nt(weights[1], key_norm)
        back = dot_nt(weights[2], values) * minus_rate
        s = jax.nn.sigmoid(gate)
        silu = gate * s
        lefts = (
            (back * up * s * (1.0 + gate * (1.0 - s)), key_norm),
            (back * silu, key_norm),
            (silu * up * minus_rate, values),
        )
        for m, (left, right) in enumerate(lefts):
            part = dot_nn(left.astype(BF16), right)
            sums[m] = part if sums[m] is None else sums[m] + part
    for m in range(3):
        out_ref[:, m] = sums[m].reshape(n, r, w).astype(BF16)


def sum_and_copy(arr_ref, out_ref):
    total = arr_ref[0].astype(F32)
    for d in range(1, arr_ref.shape[0]):
        total = total + arr_ref[d].astype(F32)
    total = total.astype(BF16)
    for d in range(out_ref.shape[0]):
        out_ref[d] = total


def slice_of(where_ref, near_ref, far_ref, out_ref):
    for ref, odd in ((near_ref, 0), (far_ref, 1)):
        for i, d in enumerate((0, 4, 2, 6)):
            out_ref[where_ref[0] ^ (d + odd)] = ref[i]


def arrange(where_ref, *refs):
    pieces, out_ref = refs[:-1], refs[-1]
    planes = pieces[0].shape[0]
    for d, piece in enumerate(pieces):
        for z in range(planes):
            out_ref[z * len(pieces) + (where_ref[1] ^ d)] = piece[z]


def in_parts(x):
    high = x.astype(BF16).astype(F32)
    middle = (x - high).astype(BF16).astype(F32)
    return high, middle, x - high - middle


def attended(where_ref, q, own_ref, other_ref, q_plane, k_plane):
    t, w = q.shape
    chips = own_ref.shape[0]
    y, core = where_ref[1], where_ref[2]
    plane = 2 * chips * t
    q_pos = q_plane * plane + (2 * y + core) * t
    q_pos = q_pos + lax.broadcasted_iota(jnp.int32, (t, chips * t), 0)
    lane = lax.broadcasted_iota(jnp.int32, (t, chips * t), 1)
    lane = lane + lane // t * t
    parts = []
    for ref, k_core in ((own_ref, core), (other_ref, 1 - core)):
        k_pos = k_plane * plane + k_core * t + lane
        seen = (k_pos <= q_pos) & (k_pos > q_pos - WINDOW) & (k_pos >= 0)
        scores = dot_nt(q, ref[:, :t].reshape(chips * t, w)) * (w ** (-0.5))
        parts.append(jnp.where(seen, scores, HIDDEN))
    top = jnp.max(jnp.maximum(parts[0], parts[1]), axis=1, keepdims=True)
    parts = [jnp.exp(p - top) for p in parts]
    total = jnp.sum(parts[0] + parts[1], axis=1, keepdims=True)
    out = jnp.zeros((t, w), F32)
    for p, ref in zip(parts, (own_ref, other_ref)):
        out = out + dot_nn(p.astype(BF16), ref[:, t : 2 * t].reshape(chips * t, w))
    return out, top, total


def attend_before(where_ref, q_ref, own_ref, other_ref, out_ref):
    q_plane = (where_ref[0] + 1) % CHIPS_Z
    out, top, total = attended(where_ref, q_ref[...], own_ref, other_ref, q_plane, q_plane - 1)
    t, w = out.shape
    out_ref[:, :w] = (out / total).astype(BF16)
    lane = lax.broadcasted_iota(jnp.int32, (t, out_ref.shape[1] - w), 1)
    extra = jnp.zeros(lane.shape, F32)
    for i, part in enumerate((*in_parts(top), *in_parts(total))):
        extra = jnp.where(lane == i, part, extra)
    out_ref[:, w:] = extra.astype(BF16)


def attend(where_ref, q_ref, own_ref, other_ref, before_ref, out_ref):
    z = where_ref[0]
    out, top, total = attended(where_ref, q_ref[...], own_ref, other_ref, z, z)
    w = out.shape[1]
    extra = before_ref[:, w:].astype(F32)
    top_before = extra[:, 0:1] + extra[:, 1:2] + extra[:, 2:3]
    total_before = extra[:, 3:4] + extra[:, 4:5] + extra[:, 5:6]
    highest = jnp.maximum(top, top_before)
    share = jnp.exp(top - highest)
    share_before = total_before * jnp.exp(top_before - highest)
    inverse = 1.0 / (total * share + share_before)
    out_ref[...] = out * (share * inverse) + before_ref[:, :w].astype(F32) * (share_before * inverse)


def newton(where_ref, rate_ref, g_own, g_other, state_ref, rows_ref, x_ref):
    _, _, r, _ = g_own.shape
    rate = rate_ref[0]
    chip = where_ref[0] * CHIPS_Y + where_ref[1]
    xs = []
    for m in range(3):
        g = jnp.concatenate([merged_rows(g_own, m), merged_rows(g_other, m)], axis=0)
        xs.append(g / (jnp.sqrt(jnp.sum(g * g, keepdims=True)) + NORM_EPS))
    for _ in range(NS_STEPS):
        lows = [x.astype(BF16) for x in xs]
        grams = [dot_nt(low, low) for low in lows]
        gram_lows = [gram.astype(BF16) for gram in grams]
        squares = [dot_nn(gram, gram) for gram in gram_lows]
        polys = [(NS_2 * gram + NS_3 * sq).astype(BF16) for gram, sq in zip(grams, squares)]
        moved = [dot_nn(poly, low) for poly, low in zip(polys, lows)]
        xs = [NS_1 * x + move for x, move in zip(xs, moved)]
    for m, x in enumerate(xs):
        x_ref[m] = x
        rows_ref[m] = state_ref[m] - rate * x_ref[m, pl.ds(pl.multiple_of(chip * r, r), r)]


def finish(rate_ref, x_ref, old_own, old_other, qn_ref, att_ref, out_ref, fresh_ref):
    n, _, r, _ = old_own.shape
    half = n * r
    rate = rate_ref[0]
    for m in range(3):
        fresh_ref[m, :half] = (merged_rows(old_own, m) - rate * x_ref[m, :half]).astype(BF16)
        fresh_ref[m, half:] = (merged_rows(old_other, m) - rate * x_ref[m, half:]).astype(BF16)
    gate = dot_nt(qn_ref[...], fresh_ref[0])
    up = dot_nt(qn_ref[...], fresh_ref[1])
    active = (jax.nn.silu(gate) * up).astype(BF16)
    out_ref[...] = (att_ref[...] + dot_nn(active, fresh_ref[2])).astype(BF16)


def join_heads(arr_ref, out_ref):
    for h in range(arr_ref.shape[0]):
        hd = arr_ref.shape[2]
        out_ref[:, h * hd : (h + 1) * hd] = arr_ref[h]


def shards(qkv, token_rate, head_rate, fast_state):
    heads = lax.axis_size("head")
    chips = CHIPS_Z * CHIPS_Y
    _, tok_part, width = qkv.shape
    hd = width // heads
    tok = tok_part * heads
    rows = fast_state.shape[2]
    where = jnp.stack([lax.axis_index(a) for a in SEQ]).astype(jnp.int32)
    state = fast_state[:, 0]
    swap = [(0, 1), (1, 0)]

    def shape(dims, dtype=BF16):
        return jax.ShapeDtypeStruct(dims, dtype)

    def exchanged(pieces, axis):
        return lax.all_to_all(pieces, axis, 0, 0, tiled=True)

    split = local_call(
        split_heads, shape((heads, 3, tok_part, hd)), (qkv,), hbm_in=(0,), hbm_out=(0,)
    )
    arrived = exchanged(split, "head")
    q, q_norm, sent = local_call(
        prepare,
        [shape((tok, hd)), shape((tok, hd)), shape((CHIPS_Y, 2 * tok + RATE_ROWS, hd))],
        (arrived, token_rate.reshape(1, tok)),
        hbm_out=(0, 1, 2),
    )
    kv_own = exchanged(sent, "y")

    q_above = lax.ppermute(q, "z", [((i + 1) % CHIPS_Z, i) for i in range(CHIPS_Z)])

    def across(distance):
        return [(i, i ^ distance) for i in range(CHIPS_Z)]

    old_two = state.astype(BF16)[None]
    old_two = jnp.concatenate([old_two, lax.ppermute(old_two, "z", across(4))])
    old_four = jnp.concatenate([old_two, lax.ppermute(old_two, "z", across(2))])
    old_far = lax.ppermute(old_four, "z", across(1))
    old_slice = local_call(
        slice_of, shape((CHIPS_Z, 3, rows, hd)), (where, old_four, old_far), smem=(0,)
    )
    kv_other = lax.ppermute(kv_own, "core", swap)
    partial = local_call(
        gradient, shape((CHIPS_Z, 3, rows, hd)), (kv_own, kv_other, old_slice), hbm_out=(0,)
    )
    parts = exchanged(partial, "z")
    g_copies = local_call(sum_and_copy, shape((chips, 3, rows, hd)), (parts,), hbm_out=(0,))
    g_own = exchanged(g_copies, CHIPS)
    share = local_call(
        attend_before,
        shape((tok, hd + 128)),
        (where, q_above, kv_own, kv_other),
        smem=(0,),
    )
    up = [(i, (i + 1) % CHIPS_Z) for i in range(CHIPS_Z)]
    before = lax.ppermute(share, "z", up)
    attention = local_call(
        attend,
        shape((tok, hd), F32),
        (where, q, kv_own, kv_other, before),
        smem=(0,),
        hbm_in=(1,),
    )
    olds = [old_slice] + [
        lax.ppermute(old_slice, "y", [(i, i ^ d) for i in range(CHIPS_Y)])
        for d in range(1, CHIPS_Y)
    ]
    old_own = local_call(arrange, shape((chips, 3, rows, hd)), (where, *olds), smem=(0,))
    old_other = lax.ppermute(old_own, "core", swap)
    g_other = lax.ppermute(g_own, "core", swap)
    new_rows, x = local_call(
        newton,
        [shape((3, rows, hd), F32), shape((3, 2 * chips * rows, hd), F32)],
        (where, head_rate, g_own, g_other, state),
        smem=(0, 1),
        hbm_in=(4,),
        hbm_out=(0,),
    )
    combined = local_call(
        finish,
        shape((tok, hd)),
        (head_rate, x, old_own, old_other, q_norm, attention),
        smem=(0,),
        hbm_in=(4,),
        hbm_out=(0,),
        scratch=[pltpu.VMEM((3, 2 * chips * rows, hd), BF16)],
    )
    back = exchanged(combined.reshape(heads, tok_part, hd), "head")
    return (
        local_call(join_heads, shape((tok_part, width)), (back,), hbm_out=(0,)),
        new_rows[:, None],
    )


def solution(mesh):
    finer = Mesh(mesh.devices.reshape(CHIPS_Z, CHIPS_Y, 2, mesh.shape["head"]), SEQ_HEAD)
    return jax.shard_map(
        shards,
        mesh=finer,
        in_specs=(P(None, SEQ_HEAD, None), P(SEQ, "head"), P("head"), P(None, "head", SEQ, None)),
        out_specs=(P(SEQ_HEAD, None), P(None, "head", SEQ, None)),
        check_vma=False,
    )
```

```python
import jax
import jax.numpy as jnp
from jax import lax
from jax.experimental import pallas as pl
from jax.experimental.pallas import tpu as pltpu
from jax.sharding import Mesh
from jax.sharding import PartitionSpec as P

WINDOW = 1024
NS_STEPS = 2
NS_1, NS_2, NS_3 = 3.4445, -4.775, 2.0315
RMS_EPS = 1e-06
NORM_EPS = 1e-07
HIDDEN = -1e30

SEQ = ("z", "y", "core")
SEQ_HEAD = ("z", "y", "core", "head")
CHIPS = ("z", "y")
F32, BF16 = jnp.float32, jnp.bfloat16
CHIPS_Z, CHIPS_Y = 8, 4
RATE_ROWS = 8
KERNEL_VMEM = 18 * 1024 * 1024


def dot_nt(a, b):
    return lax.dot_general(a, b, (((1,), (1,)), ((), ())), preferred_element_type=F32)


def dot_nn(a, b):
    return lax.dot_general(a, b, (((1,), (0,)), ((), ())), preferred_element_type=F32)


def local_call(body, outs, args, smem=(), scratch=(), hbm_in=(), hbm_out=()):
    specs = [
        pl.BlockSpec(memory_space=pltpu.SMEM if i in smem else pltpu.VMEM) for i in range(len(args))
    ]
    single = not isinstance(outs, (list, tuple))
    out_list = [outs] if single else list(outs)
    out_list = [
        (pltpu.HBM if i in hbm_out else pltpu.VMEM)(o.shape, o.dtype)
        for i, o in enumerate(out_list)
    ]
    args = [
        a if i in smem or i in hbm_in else pltpu.with_memory_space_constraint(a, pltpu.VMEM)
        for i, a in enumerate(args)
    ]
    out_specs = [pl.BlockSpec(memory_space=pltpu.VMEM) for _ in out_list]
    return pl.pallas_call(
        body,
        in_specs=specs,
        out_specs=out_specs[0] if single else out_specs,
        out_shape=out_list[0] if single else out_list,
        scratch_shapes=list(scratch),
        compiler_params=pltpu.CompilerParams(vmem_limit_bytes=KERNEL_VMEM),
    )(*args)


def split_heads(qkv_ref, out_ref):
    for h in range(out_ref.shape[0]):
        hd = out_ref.shape[3]
        for j in range(3):
            out_ref[h, j] = qkv_ref[j, :, h * hd : (h + 1) * hd]


def rms_scaled(x):
    return x * lax.rsqrt(jnp.mean(x * x, axis=-1, keepdims=True) + RMS_EPS)


def prepare(arr_ref, rate_ref, q_ref, qn_ref, sent_ref):
    n, _, t, _ = arr_ref.shape
    copies, lines, w = sent_ref.shape
    tok = n * t
    rate = rate_ref[...]
    high, middle, low = in_parts(rate)
    spare = jnp.zeros((1, w - 3 * tok), F32)
    rate_rows = jnp.broadcast_to(
        jnp.concatenate([high, middle, low, spare], axis=1), (lines - 2 * tok, w)
    ).astype(BF16)
    for j in range(n):
        rows = slice(j * t, (j + 1) * t)
        q = arr_ref[j, 0]
        q_ref[rows] = q
        qn_ref[rows] = rms_scaled(q.astype(F32)).astype(BF16)
    for d in range(copies):
        for j in range(n):
            sent_ref[d, j * t : (j + 1) * t] = arr_ref[j, 1]
            sent_ref[d, tok + j * t : tok + (j + 1) * t] = arr_ref[j, 2]
        sent_ref[d, 2 * tok :] = rate_rows


def merged_rows(ref, m):
    n, _, r, w = ref.shape
    return ref[:, m].astype(F32).reshape(n * r, w)


def gradient(own_ref, other_ref, w_ref, out_ref):
    n, _, r, w = w_ref.shape
    weights = [merged_rows(w_ref, m).astype(BF16) for m in range(3)]
    chips, lines, _ = own_ref.shape
    tok = (lines - RATE_ROWS) // 2
    sums = [None, None, None]
    for ref in (own_ref, other_ref):
        keys = ref[:, :tok].reshape(chips * tok, w)
        values = ref[:, tok : 2 * tok].reshape(chips * tok, w)
        rates = []
        for i in range(chips):
            parts = ref[i, 2 * tok :].astype(F32)[:1]
            rates.append(parts[:, :tok] + parts[:, tok : 2 * tok] + parts[:, 2 * tok : 3 * tok])
        minus_rate = -jnp.concatenate(rates, axis=1)
        key_norm = rms_scaled(keys.astype(F32)).astype(BF16)
        gate = dot_nt(weights[0], key_norm)
        up = dot_nt(weights[1], key_norm)
        back = dot_nt(weights[2], values) * minus_rate
        s = jax.nn.sigmoid(gate)
        silu = gate * s
        lefts = (
            (back * up * s * (1.0 + gate * (1.0 - s)), key_norm),
            (back * silu, key_norm),
            (silu * up * minus_rate, values),
        )
        for m, (left, right) in enumerate(lefts):
            part = dot_nn(left.astype(BF16), right)
            sums[m] = part if sums[m] is None else sums[m] + part
    for m in range(3):
        out_ref[:, m] = sums[m].reshape(n, r, w).astype(BF16)


def sum_and_copy(arr_ref, out_ref):
    total = arr_ref[0].astype(F32)
    for d in range(1, arr_ref.shape[0]):
        total = total + arr_ref[d].astype(F32)
    total = total.astype(BF16)
    for d in range(out_ref.shape[0]):
        out_ref[d] = total


def slice_of(where_ref, near_ref, far_ref, out_ref):
    _, mats, r, w = near_ref.shape
    for i, d in enumerate((0, 4, 2, 6)):
        out_ref[(where_ref[0] + d) % CHIPS_Z] = near_ref[i]
        rows = far_ref[i * mats * r : (i + 1) * mats * r].astype(F32).reshape(mats, r, w)
        out_ref[(where_ref[0] + d + 1) % CHIPS_Z] = rows.astype(BF16)


def arrange(where_ref, *refs):
    pieces, out_ref = refs[:-1], refs[-1]
    planes = pieces[0].shape[0]
    for d, piece in enumerate(pieces):
        for z in range(planes):
            out_ref[z * len(pieces) + (where_ref[1] ^ d)] = piece[z]


def in_parts(x):
    high = x.astype(BF16).astype(F32)
    middle = (x - high).astype(BF16).astype(F32)
    return high, middle, x - high - middle


def attended(where_ref, q, own_ref, other_ref, q_plane, k_plane):
    t, w = q.shape
    chips = own_ref.shape[0]
    y, core = where_ref[1], where_ref[2]
    plane = 2 * chips * t
    q_pos = q_plane * plane + (2 * y + core) * t
    q_pos = q_pos + lax.broadcasted_iota(jnp.int32, (t, chips * t), 0)
    lane = lax.broadcasted_iota(jnp.int32, (t, chips * t), 1)
    lane = lane + lane // t * t
    parts = []
    for ref, k_core in ((own_ref, core), (other_ref, 1 - core)):
        k_pos = k_plane * plane + k_core * t + lane
        seen = (k_pos <= q_pos) & (k_pos > q_pos - WINDOW) & (k_pos >= 0)
        scores = dot_nt(q, ref[:, :t].reshape(chips * t, w)) * (w ** (-0.5))
        parts.append(jnp.where(seen, scores, HIDDEN))
    top = jnp.max(jnp.maximum(parts[0], parts[1]), axis=1, keepdims=True)
    parts = [jnp.exp(p - top) for p in parts]
    total = jnp.sum(parts[0] + parts[1], axis=1, keepdims=True)
    out = jnp.zeros((t, w), F32)
    for p, ref in zip(parts, (own_ref, other_ref)):
        out = out + dot_nn(p.astype(BF16), ref[:, t : 2 * t].reshape(chips * t, w))
    return out, top, total


def attend_before(where_ref, q_ref, own_ref, other_ref, out_ref):
    q_plane = (where_ref[0] + 1) % CHIPS_Z
    q = q_ref[q_ref.shape[0] - out_ref.shape[0] :]
    out, top, total = attended(where_ref, q, own_ref, other_ref, q_plane, q_plane - 1)
    t, w = out.shape
    out_ref[:, :w] = (out / total).astype(BF16)
    lane = lax.broadcasted_iota(jnp.int32, (t, out_ref.shape[1] - w), 1)
    extra = jnp.zeros(lane.shape, F32)
    for i, part in enumerate((*in_parts(top), *in_parts(total))):
        extra = jnp.where(lane == i, part, extra)
    out_ref[:, w:] = extra.astype(BF16)


def attend(where_ref, q_ref, own_ref, other_ref, before_ref, out_ref):
    z = where_ref[0]
    out, top, total = attended(where_ref, q_ref[...], own_ref, other_ref, z, z)
    w = out.shape[1]
    extra = before_ref[:, w:].astype(F32)
    top_before = extra[:, 0:1] + extra[:, 1:2] + extra[:, 2:3]
    total_before = extra[:, 3:4] + extra[:, 4:5] + extra[:, 5:6]
    highest = jnp.maximum(top, top_before)
    share = jnp.exp(top - highest)
    share_before = total_before * jnp.exp(top_before - highest)
    inverse = 1.0 / (total * share + share_before)
    out_ref[...] = out * (share * inverse) + before_ref[:, :w].astype(F32) * (share_before * inverse)


def newton(where_ref, rate_ref, g_own, g_other, state_ref, rows_ref, x_ref):
    _, _, r, _ = g_own.shape
    rate = rate_ref[0]
    chip = where_ref[0] * CHIPS_Y + where_ref[1]
    xs = []
    for m in range(3):
        g = jnp.concatenate([merged_rows(g_own, m), merged_rows(g_other, m)], axis=0)
        xs.append(g / (jnp.sqrt(jnp.sum(g * g, keepdims=True)) + NORM_EPS))
    for _ in range(NS_STEPS):
        lows = [x.astype(BF16) for x in xs]
        grams = [dot_nt(low, low) for low in lows]
        gram_lows = [gram.astype(BF16) for gram in grams]
        squares = [dot_nn(gram, gram) for gram in gram_lows]
        polys = [(NS_2 * gram + NS_3 * sq).astype(BF16) for gram, sq in zip(grams, squares)]
        moved = [dot_nn(poly, low) for poly, low in zip(polys, lows)]
        xs = [NS_1 * x + move for x, move in zip(xs, moved)]
    for m, x in enumerate(xs):
        x_ref[m] = x
        rows_ref[m] = state_ref[m] - rate * x_ref[m, pl.ds(pl.multiple_of(chip * r, r), r)]


def finish(rate_ref, x_ref, old_own, old_other, qn_ref, att_ref, out_ref, fresh_ref):
    n, _, r, _ = old_own.shape
    half = n * r
    rate = rate_ref[0]
    for m in range(3):
        fresh_ref[m, :half] = (merged_rows(old_own, m) - rate * x_ref[m, :half]).astype(BF16)
        fresh_ref[m, half:] = (merged_rows(old_other, m) - rate * x_ref[m, half:]).astype(BF16)
    gate = dot_nt(qn_ref[...], fresh_ref[0])
    up = dot_nt(qn_ref[...], fresh_ref[1])
    active = (jax.nn.silu(gate) * up).astype(BF16)
    out_ref[...] = (att_ref[...] + dot_nn(active, fresh_ref[2])).astype(BF16)


def join_heads(arr_ref, out_ref):
    for h in range(arr_ref.shape[0]):
        hd = arr_ref.shape[2]
        out_ref[:, h * hd : (h + 1) * hd] = arr_ref[h]


def shards(qkv, token_rate, head_rate, fast_state):
    heads = lax.axis_size("head")
    chips = CHIPS_Z * CHIPS_Y
    _, tok_part, width = qkv.shape
    hd = width // heads
    tok = tok_part * heads
    rows = fast_state.shape[2]
    where = jnp.stack([lax.axis_index(a) for a in SEQ]).astype(jnp.int32)
    state = fast_state[:, 0]
    swap = [(0, 1), (1, 0)]

    def shape(dims, dtype=BF16):
        return jax.ShapeDtypeStruct(dims, dtype)

    def exchanged(pieces, axis):
        return lax.all_to_all(pieces, axis, 0, 0, tiled=True)

    split = local_call(
        split_heads, shape((heads, 3, tok_part, hd)), (qkv,), hbm_in=(0,), hbm_out=(0,)
    )
    arrived = exchanged(split, "head")
    q, q_norm, sent = local_call(
        prepare,
        [shape((tok, hd)), shape((tok, hd)), shape((CHIPS_Y, 2 * tok + RATE_ROWS, hd))],
        (arrived, token_rate.reshape(1, tok)),
        hbm_out=(0, 1, 2),
    )
    kv_own = exchanged(sent, "y")

    def above(distance):
        return [((i + distance) % CHIPS_Z, i) for i in range(CHIPS_Z)]

    old_two = state.astype(BF16)[None]
    old_two = jnp.concatenate([old_two, lax.ppermute(old_two, "z", above(4))])
    old_four = jnp.concatenate([old_two, lax.ppermute(old_two, "z", above(2))])
    sent_down = jnp.concatenate([old_four.reshape(-1, hd), q])
    old_far = lax.ppermute(sent_down, "z", above(1))
    old_slice = local_call(
        slice_of, shape((CHIPS_Z, 3, rows, hd)), (where, old_four, old_far), smem=(0,)
    )
    kv_other = lax.ppermute(kv_own, "core", swap)
    partial = local_call(
        gradient, shape((CHIPS_Z, 3, rows, hd)), (kv_own, kv_other, old_slice), hbm_out=(0,)
    )
    parts = exchanged(partial, "z")
    g_copies = local_call(sum_and_copy, shape((chips, 3, rows, hd)), (parts,), hbm_out=(0,))
    g_own = exchanged(g_copies, CHIPS)
    share = local_call(
        attend_before,
        shape((tok, hd + 128)),
        (where, old_far, kv_own, kv_other),
        smem=(0,),
    )
    up = [(i, (i + 1) % CHIPS_Z) for i in range(CHIPS_Z)]
    before = lax.ppermute(share, "z", up)
    attention = local_call(
        attend,
        shape((tok, hd), F32),
        (where, q, kv_own, kv_other, before),
        smem=(0,),
        hbm_in=(1,),
    )
    olds = [old_slice] + [
        lax.ppermute(old_slice, "y", [(i, i ^ d) for i in range(CHIPS_Y)])
        for d in range(1, CHIPS_Y)
    ]
    old_own = local_call(arrange, shape((chips, 3, rows, hd)), (where, *olds), smem=(0,))
    old_other = lax.ppermute(old_own, "core", swap)
    g_other = lax.ppermute(g_own, "core", swap)
    new_rows, x = local_call(
        newton,
        [shape((3, rows, hd), F32), shape((3, 2 * chips * rows, hd), F32)],
        (where, head_rate, g_own, g_other, state),
        smem=(0, 1),
        hbm_in=(4,),
        hbm_out=(0,),
    )
    combined = local_call(
        finish,
        shape((tok, hd)),
        (head_rate, x, old_own, old_other, q_norm, attention),
        smem=(0,),
        hbm_in=(4,),
        hbm_out=(0,),
        scratch=[pltpu.VMEM((3, 2 * chips * rows, hd), BF16)],
    )
    back = exchanged(combined.reshape(heads, tok_part, hd), "head")
    return (
        local_call(join_heads, shape((tok_part, width)), (back,), hbm_out=(0,)),
        new_rows[:, None],
    )


def solution(mesh):
    finer = Mesh(mesh.devices.reshape(CHIPS_Z, CHIPS_Y, 2, mesh.shape["head"]), SEQ_HEAD)
    return jax.shard_map(
        shards,
        mesh=finer,
        in_specs=(P(None, SEQ_HEAD, None), P(SEQ, "head"), P("head"), P(None, "head", SEQ, None)),
        out_specs=(P(SEQ_HEAD, None), P(None, "head", SEQ, None)),
        check_vma=False,
    )
```

```python
import jax
import jax.numpy as jnp
from jax import lax
from jax.experimental import pallas as pl
from jax.experimental.pallas import tpu as pltpu
from jax.sharding import Mesh
from jax.sharding import PartitionSpec as P

WINDOW = 1024
NS_STEPS = 2
NS_1, NS_2, NS_3 = 3.4445, -4.775, 2.0315
RMS_EPS = 1e-06
NORM_EPS = 1e-07
HIDDEN = -1e30

SEQ = ("z", "y", "core")
SEQ_HEAD = ("z", "y", "core", "head")
CHIPS = ("z", "y")
F32, BF16 = jnp.float32, jnp.bfloat16
CHIPS_Z, CHIPS_Y = 8, 4
RATE_ROWS = 8
KERNEL_VMEM = 9 * 1024 * 1024
NEWTON_VMEM = 18 * 1024 * 1024


def dot_nt(a, b):
    return lax.dot_general(a, b, (((1,), (1,)), ((), ())), preferred_element_type=F32)


def dot_nn(a, b):
    return lax.dot_general(a, b, (((1,), (0,)), ((), ())), preferred_element_type=F32)


def local_call(body, outs, args, smem=(), scratch=(), hbm_in=(), hbm_out=(), vmem=KERNEL_VMEM):
    specs = [
        pl.BlockSpec(memory_space=pltpu.SMEM if i in smem else pltpu.VMEM) for i in range(len(args))
    ]
    single = not isinstance(outs, (list, tuple))
    out_list = [outs] if single else list(outs)
    out_list = [
        (pltpu.HBM if i in hbm_out else pltpu.VMEM)(o.shape, o.dtype)
        for i, o in enumerate(out_list)
    ]
    args = [
        a if i in smem or i in hbm_in else pltpu.with_memory_space_constraint(a, pltpu.VMEM)
        for i, a in enumerate(args)
    ]
    out_specs = [pl.BlockSpec(memory_space=pltpu.VMEM) for _ in out_list]
    return pl.pallas_call(
        body,
        in_specs=specs,
        out_specs=out_specs[0] if single else out_specs,
        out_shape=out_list[0] if single else out_list,
        scratch_shapes=list(scratch),
        compiler_params=pltpu.CompilerParams(vmem_limit_bytes=vmem),
    )(*args)


def split_heads(qkv_ref, out_ref):
    for h in range(out_ref.shape[0]):
        hd = out_ref.shape[3]
        for j in range(3):
            out_ref[h, j] = qkv_ref[j, :, h * hd : (h + 1) * hd]


def rms_scaled(x):
    return x * lax.rsqrt(jnp.mean(x * x, axis=-1, keepdims=True) + RMS_EPS)


def prepare(arr_ref, rate_ref, q_ref, qn_ref, sent_ref):
    n, _, t, _ = arr_ref.shape
    copies, lines, w = sent_ref.shape
    tok = n * t
    rate = rate_ref[...]
    high, middle, low = in_parts(rate)
    spare = jnp.zeros((1, w - 3 * tok), F32)
    rate_rows = jnp.broadcast_to(
        jnp.concatenate([high, middle, low, spare], axis=1), (lines - 2 * tok, w)
    ).astype(BF16)
    for j in range(n):
        rows = slice(j * t, (j + 1) * t)
        q = arr_ref[j, 0]
        q_ref[rows] = q
        qn_ref[rows] = rms_scaled(q.astype(F32)).astype(BF16)
    for d in range(copies):
        for j in range(n):
            sent_ref[d, j * t : (j + 1) * t] = arr_ref[j, 1]
            sent_ref[d, tok + j * t : tok + (j + 1) * t] = arr_ref[j, 2]
        sent_ref[d, 2 * tok :] = rate_rows


def merged_rows(ref, m):
    n, _, r, w = ref.shape
    return ref[:, m].astype(F32).reshape(n * r, w)


def gradient(own_ref, other_ref, w_ref, out_ref):
    n, _, r, w = w_ref.shape
    weights = [merged_rows(w_ref, m).astype(BF16) for m in range(3)]
    chips, lines, _ = own_ref.shape
    tok = (lines - RATE_ROWS) // 2
    sums = [None, None, None]
    for ref in (own_ref, other_ref):
        keys = ref[:, :tok].reshape(chips * tok, w)
        values = ref[:, tok : 2 * tok].reshape(chips * tok, w)
        rates = []
        for i in range(chips):
            parts = ref[i, 2 * tok :].astype(F32)[:1]
            rates.append(parts[:, :tok] + parts[:, tok : 2 * tok] + parts[:, 2 * tok : 3 * tok])
        minus_rate = -jnp.concatenate(rates, axis=1)
        key_norm = rms_scaled(keys.astype(F32)).astype(BF16)
        gate = dot_nt(weights[0], key_norm)
        up = dot_nt(weights[1], key_norm)
        back = dot_nt(weights[2], values) * minus_rate
        s = jax.nn.sigmoid(gate)
        silu = gate * s
        lefts = (
            (back * up * s * (1.0 + gate * (1.0 - s)), key_norm),
            (back * silu, key_norm),
            (silu * up * minus_rate, values),
        )
        for m, (left, right) in enumerate(lefts):
            part = dot_nn(left.astype(BF16), right)
            sums[m] = part if sums[m] is None else sums[m] + part
    for m in range(3):
        out_ref[:, m] = sums[m].reshape(n, r, w).astype(BF16)


def sum_and_copy(arr_ref, out_ref):
    total = arr_ref[0].astype(F32)
    for d in range(1, arr_ref.shape[0]):
        total = total + arr_ref[d].astype(F32)
    total = total.astype(BF16)
    for d in range(out_ref.shape[0]):
        out_ref[d] = total


def slice_of(where_ref, near_ref, far_ref, out_ref):
    _, mats, r, w = near_ref.shape
    for i, d in enumerate((0, 4, 2, 6)):
        out_ref[(where_ref[0] + d) % CHIPS_Z] = near_ref[i]
        rows = far_ref[i * mats * r : (i + 1) * mats * r].astype(F32).reshape(mats, r, w)
        out_ref[(where_ref[0] + d + 1) % CHIPS_Z] = rows.astype(BF16)


def arrange(where_ref, *refs):
    pieces, out_ref = refs[:-1], refs[-1]
    planes = pieces[0].shape[0]
    for d, piece in enumerate(pieces):
        for z in range(planes):
            out_ref[z * len(pieces) + (where_ref[1] ^ d)] = piece[z]


def in_parts(x):
    high = x.astype(BF16).astype(F32)
    middle = (x - high).astype(BF16).astype(F32)
    return high, middle, x - high - middle


def attended(where_ref, q, own_ref, other_ref, q_plane, k_plane):
    t, w = q.shape
    chips = own_ref.shape[0]
    y, core = where_ref[1], where_ref[2]
    plane = 2 * chips * t
    q_pos = q_plane * plane + (2 * y + core) * t
    q_pos = q_pos + lax.broadcasted_iota(jnp.int32, (t, chips * t), 0)
    lane = lax.broadcasted_iota(jnp.int32, (t, chips * t), 1)
    lane = lane + lane // t * t
    parts = []
    for ref, k_core in ((own_ref, core), (other_ref, 1 - core)):
        k_pos = k_plane * plane + k_core * t + lane
        seen = (k_pos <= q_pos) & (k_pos > q_pos - WINDOW) & (k_pos >= 0)
        scores = dot_nt(q, ref[:, :t].reshape(chips * t, w)) * (w ** (-0.5))
        parts.append(jnp.where(seen, scores, HIDDEN))
    top = jnp.max(jnp.maximum(parts[0], parts[1]), axis=1, keepdims=True)
    parts = [jnp.exp(p - top) for p in parts]
    total = jnp.sum(parts[0] + parts[1], axis=1, keepdims=True)
    out = jnp.zeros((t, w), F32)
    for p, ref in zip(parts, (own_ref, other_ref)):
        out = out + dot_nn(p.astype(BF16), ref[:, t : 2 * t].reshape(chips * t, w))
    return out, top, total


def attend_before(where_ref, q_ref, own_ref, other_ref, out_ref):
    q_plane = (where_ref[0] + 1) % CHIPS_Z
    q = q_ref[q_ref.shape[0] - out_ref.shape[0] :]
    out, top, total = attended(where_ref, q, own_ref, other_ref, q_plane, q_plane - 1)
    t, w = out.shape
    out_ref[:, :w] = (out / total).astype(BF16)
    lane = lax.broadcasted_iota(jnp.int32, (t, out_ref.shape[1] - w), 1)
    extra = jnp.zeros(lane.shape, F32)
    for i, part in enumerate((*in_parts(top), *in_parts(total))):
        extra = jnp.where(lane == i, part, extra)
    out_ref[:, w:] = extra.astype(BF16)


def attend(where_ref, q_ref, own_ref, other_ref, before_ref, out_ref):
    z = where_ref[0]
    out, top, total = attended(where_ref, q_ref[...], own_ref, other_ref, z, z)
    w = out.shape[1]
    extra = before_ref[:, w:].astype(F32)
    top_before = extra[:, 0:1] + extra[:, 1:2] + extra[:, 2:3]
    total_before = extra[:, 3:4] + extra[:, 4:5] + extra[:, 5:6]
    highest = jnp.maximum(top, top_before)
    share = jnp.exp(top - highest)
    share_before = total_before * jnp.exp(top_before - highest)
    inverse = 1.0 / (total * share + share_before)
    out_ref[...] = out * (share * inverse) + before_ref[:, :w].astype(F32) * (share_before * inverse)


def newton(where_ref, rate_ref, g_own, g_other, state_ref, rows_ref, x_ref):
    _, _, r, _ = g_own.shape
    rate = rate_ref[0]
    chip = where_ref[0] * CHIPS_Y + where_ref[1]
    xs = []
    for m in range(3):
        g = jnp.concatenate([merged_rows(g_own, m), merged_rows(g_other, m)], axis=0)
        xs.append(g / (jnp.sqrt(jnp.sum(g * g, keepdims=True)) + NORM_EPS))
    for _ in range(NS_STEPS):
        lows = [x.astype(BF16) for x in xs]
        grams = [dot_nt(low, low) for low in lows]
        gram_lows = [gram.astype(BF16) for gram in grams]
        squares = [dot_nn(gram, gram) for gram in gram_lows]
        polys = [(NS_2 * gram + NS_3 * sq).astype(BF16) for gram, sq in zip(grams, squares)]
        moved = [dot_nn(poly, low) for poly, low in zip(polys, lows)]
        xs = [NS_1 * x + move for x, move in zip(xs, moved)]
    for m, x in enumerate(xs):
        x_ref[m] = x
        rows_ref[m] = state_ref[m] - rate * x_ref[m, pl.ds(pl.multiple_of(chip * r, r), r)]


def finish(rate_ref, x_ref, old_own, old_other, qn_ref, att_ref, out_ref, fresh_ref):
    n, _, r, _ = old_own.shape
    half = n * r
    rate = rate_ref[0]
    for m in range(3):
        fresh_ref[m, :half] = (merged_rows(old_own, m) - rate * x_ref[m, :half]).astype(BF16)
        fresh_ref[m, half:] = (merged_rows(old_other, m) - rate * x_ref[m, half:]).astype(BF16)
    gate = dot_nt(qn_ref[...], fresh_ref[0])
    up = dot_nt(qn_ref[...], fresh_ref[1])
    active = (jax.nn.silu(gate) * up).astype(BF16)
    out_ref[...] = (att_ref[...] + dot_nn(active, fresh_ref[2])).astype(BF16)


def join_heads(arr_ref, out_ref):
    for h in range(arr_ref.shape[0]):
        hd = arr_ref.shape[2]
        out_ref[:, h * hd : (h + 1) * hd] = arr_ref[h]


def shards(qkv, token_rate, head_rate, fast_state):
    heads = lax.axis_size("head")
    chips = CHIPS_Z * CHIPS_Y
    _, tok_part, width = qkv.shape
    hd = width // heads
    tok = tok_part * heads
    rows = fast_state.shape[2]
    where = jnp.stack([lax.axis_index(a) for a in SEQ]).astype(jnp.int32)
    state = fast_state[:, 0]
    swap = [(0, 1), (1, 0)]

    def shape(dims, dtype=BF16):
        return jax.ShapeDtypeStruct(dims, dtype)

    def exchanged(pieces, axis):
        return lax.all_to_all(pieces, axis, 0, 0, tiled=True)

    split = local_call(
        split_heads, shape((heads, 3, tok_part, hd)), (qkv,), hbm_in=(0,), hbm_out=(0,)
    )
    arrived = exchanged(split, "head")
    q, q_norm, sent = local_call(
        prepare,
        [shape((tok, hd)), shape((tok, hd)), shape((CHIPS_Y, 2 * tok + RATE_ROWS, hd))],
        (arrived, token_rate.reshape(1, tok)),
        hbm_out=(0, 1, 2),
    )
    kv_own = exchanged(sent, "y")

    def above(distance):
        return [((i + distance) % CHIPS_Z, i) for i in range(CHIPS_Z)]

    old_two = state.astype(BF16)[None]
    old_two = jnp.concatenate([old_two, lax.ppermute(old_two, "z", above(4))])
    old_four = jnp.concatenate([old_two, lax.ppermute(old_two, "z", above(2))])
    sent_down = jnp.concatenate([old_four.reshape(-1, hd), q])
    old_far = lax.ppermute(sent_down, "z", above(1))
    old_slice = local_call(
        slice_of, shape((CHIPS_Z, 3, rows, hd)), (where, old_four, old_far), smem=(0,)
    )
    kv_other = lax.ppermute(kv_own, "core", swap)
    partial = local_call(
        gradient, shape((CHIPS_Z, 3, rows, hd)), (kv_own, kv_other, old_slice), hbm_out=(0,)
    )
    parts = exchanged(partial, "z")
    g_copies = local_call(sum_and_copy, shape((chips, 3, rows, hd)), (parts,), hbm_out=(0,))
    g_own = exchanged(g_copies, CHIPS)
    share = local_call(
        attend_before,
        shape((tok, hd + 128)),
        (where, old_far, kv_own, kv_other),
        smem=(0,),
    )
    up = [(i, (i + 1) % CHIPS_Z) for i in range(CHIPS_Z)]
    before = lax.ppermute(share, "z", up)
    attention = local_call(
        attend,
        shape((tok, hd), F32),
        (where, q, kv_own, kv_other, before),
        smem=(0,),
        hbm_in=(1,),
    )
    olds = [old_slice] + [
        lax.ppermute(old_slice, "y", [(i, i ^ d) for i in range(CHIPS_Y)])
        for d in range(1, CHIPS_Y)
    ]
    old_own = local_call(arrange, shape((chips, 3, rows, hd)), (where, *olds), smem=(0,))
    old_other = lax.ppermute(old_own, "core", swap)
    g_other = lax.ppermute(g_own, "core", swap)
    new_rows, x = local_call(
        newton,
        [shape((3, rows, hd), F32), shape((3, 2 * chips * rows, hd), F32)],
        (where, head_rate, g_own, g_other, state),
        smem=(0, 1),
        hbm_in=(4,),
        hbm_out=(0,),
        vmem=NEWTON_VMEM,
    )
    combined = local_call(
        finish,
        shape((tok, hd)),
        (head_rate, x, old_own, old_other, q_norm, attention),
        smem=(0,),
        hbm_in=(4,),
        hbm_out=(0,),
        scratch=[pltpu.VMEM((3, 2 * chips * rows, hd), BF16)],
    )
    back = exchanged(combined.reshape(heads, tok_part, hd), "head")
    return (
        local_call(join_heads, shape((tok_part, width)), (back,), hbm_out=(0,)),
        new_rows[:, None],
    )


def solution(mesh):
    finer = Mesh(mesh.devices.reshape(CHIPS_Z, CHIPS_Y, 2, mesh.shape["head"]), SEQ_HEAD)
    return jax.shard_map(
        shards,
        mesh=finer,
        in_specs=(P(None, SEQ_HEAD, None), P(SEQ, "head"), P("head"), P(None, "head", SEQ, None)),
        out_specs=(P(SEQ_HEAD, None), P(None, "head", SEQ, None)),
        check_vma=False,
    )
```
